32 devices in a mesh: dp: 1 (over z), cp: 32 (over y, x, core).
Axes of the slice: x: 4, y: 4, z: 1, core: 2. Of those that a mesh axis runs over, the one named last changes fastest.
The devices are a block of a 4x4x8 slice.
Arguments:
- x_norm: bfloat16 [4096, 2048], P(('dp', 'cp'))
- y_grad: bfloat16 [4096, 2048], P(('dp', 'cp'))
- w_q: bfloat16 [2048, 16, 192], replicated
- w_dkv: bfloat16 [2048, 512], replicated
- g_kv: bfloat16 [512], replicated
- w_kr: bfloat16 [2048, 64], replicated
- w_uk: bfloat16 [512, 16, 128], replicated
- w_uv: bfloat16 [512, 16, 128], replicated
- w_o: bfloat16 [16, 128, 2048], replicated
Outputs:
- output 1: bfloat16 [4096, 2048], P(('dp', 'cp'))
- output 2: bfloat16 [4096, 2048], P(('dp', 'cp'))
- output 3: float32 [2048, 16, 192], P('dp')
- output 4: float32 [2048, 512], P('dp')
- output 5: float32 [512], P('dp')
- output 6: float32 [2048, 64], P('dp')
- output 7: float32 [512, 16, 128], P('dp')
- output 8: float32 [512, 16, 128], P('dp')
- output 9: float32 [16, 128, 2048], P('dp')
All inputs are finite; a program needn't handle non-finite values.
Results may differ from the reference program's by a relative error of at most 0.02.
Values are sent between devices in bfloat16 or wider.
A program may use at most 768 MiB of HBM per device.

```python
import jax
import jax.numpy as jnp
from jax import lax

D = 2048
HEADS = 16
KV_RANK = 512
NOPE = 128
ROPE = 64
VDIM = 128
SEQ = 4096
QBLK = 64
QK_DIM = NOPE + ROPE
ROPE_THETA = 10000.0
NORM_EPS = 1e-6


def setup_inputs(seed: int = 0, part: int = 0) -> dict:
    part_key = jax.random.fold_in(jax.random.key(seed), part)
    key_x, key_gy = jax.random.split(part_key, 2)
    weight_keys = jax.random.split(jax.random.key(seed + 1), 7)
    o_scale = (HEADS * VDIM) ** -0.5 * SEQ ** 0.5 / 6.0
    x_norm = jax.random.normal(key_x, (SEQ, D), jnp.float32)
    y_grad = jax.random.normal(key_gy, (SEQ, D), jnp.float32)
    w_q = jax.random.normal(weight_keys[0], (D, HEADS, QK_DIM), jnp.float32) * (1.5 * D ** -0.5)
    w_dkv = jax.random.normal(weight_keys[1], (D, KV_RANK), jnp.float32) * D ** -0.5
    g_kv = 1.0 + 0.3 * jax.random.normal(weight_keys[2], (KV_RANK,), jnp.float32)
    w_kr = jax.random.normal(weight_keys[3], (D, ROPE), jnp.float32) * D ** -0.5
    w_uk = jax.random.normal(weight_keys[4], (KV_RANK, HEADS, NOPE), jnp.float32) * KV_RANK ** -0.5
    w_uv = jax.random.normal(weight_keys[5], (KV_RANK, HEADS, VDIM), jnp.float32) * KV_RANK ** -0.5
    w_o = jax.random.normal(weight_keys[6], (HEADS, VDIM, D), jnp.float32) * o_scale
    return {'x_norm': x_norm.astype(jnp.bfloat16), 'y_grad': y_grad.astype(jnp.bfloat16), 'w_q': w_q.astype(jnp.bfloat16), 'w_dkv': w_dkv.astype(jnp.bfloat16), 'g_kv': g_kv.astype(jnp.bfloat16), 'w_kr': w_kr.astype(jnp.bfloat16), 'w_uk': w_uk.astype(jnp.bfloat16), 'w_uv': w_uv.astype(jnp.bfloat16), 'w_o': w_o.astype(jnp.bfloat16)}


def bf16_straight(t_in):
    return t_in + lax.stop_gradient(t_in.astype(jnp.bfloat16).astype(jnp.float32) - t_in)


def rope_apply(t_in, cos_t, sin_t):
    half_dim = ROPE // 2
    first_half = t_in[..., :half_dim]
    second_half = t_in[..., half_dim:]
    return jnp.concatenate([first_half * cos_t - second_half * sin_t, second_half * cos_t + first_half * sin_t], axis=-1)


def attention_forward(x_in, w_q, w_dkv, g_kv, w_kr, w_uk, w_uv, w_o):
    inv_freq = ROPE_THETA ** (-(jnp.arange(ROPE // 2, dtype=jnp.float32) * 2.0 / ROPE))
    angles = jnp.arange(SEQ, dtype=jnp.float32)[:, None] * inv_freq[None, :]
    cos_t = jnp.cos(angles)
    sin_t = jnp.sin(angles)
    q_full = jnp.einsum('td,dhe->the', x_in, w_q)
    q_nope = bf16_straight(q_full[..., :NOPE])
    q_rope = bf16_straight(rope_apply(q_full[..., NOPE:], cos_t[:, None, :], sin_t[:, None, :]))
    c_raw = jnp.dot(x_in, w_dkv)
    inv_rms = lax.rsqrt(jnp.mean(c_raw * c_raw, axis=-1, keepdims=True) + NORM_EPS)
    latent = bf16_straight(c_raw * inv_rms * g_kv)
    k_rope = bf16_straight(rope_apply(jnp.dot(x_in, w_kr), cos_t, sin_t))
    k_nope = bf16_straight(jnp.einsum('tc,chn->thn', latent, w_uk))
    values = bf16_straight(jnp.einsum('tc,chv->thv', latent, w_uv))
    attn_scale = QK_DIM ** -0.5
    key_pos = jnp.arange(SEQ)

    def block_attn(block_args):
        qn_blk, qr_blk, blk_start = block_args
        scores = (jnp.einsum('qhn,khn->hqk', qn_blk, k_nope) + jnp.einsum('qhr,kr->hqk', qr_blk, k_rope)) * attn_scale
        causal = (blk_start + jnp.arange(QBLK))[:, None] >= key_pos[None, :]
        scores = jnp.where(causal[None], scores, -1e30)
        return jnp.einsum('hqk,khv->qhv', jax.nn.softmax(scores, axis=-1), values)

    num_blocks = SEQ // QBLK
    attn = lax.map(jax.checkpoint(block_attn), (q_nope.reshape(num_blocks, QBLK, HEADS, NOPE), q_rope.reshape(num_blocks, QBLK, HEADS, ROPE), jnp.arange(num_blocks) * QBLK))
    attn = bf16_straight(attn.reshape(SEQ, HEADS, VDIM))
    return jnp.einsum('thv,hvd->td', attn, w_o)


def reference(x_norm, y_grad, w_q, w_dkv, g_kv, w_kr, w_uk, w_uv, w_o):
    y_full, pullback = jax.vjp(attention_forward, x_norm.astype(jnp.float32), w_q.astype(jnp.float32), w_dkv.astype(jnp.float32), g_kv.astype(jnp.float32), w_kr.astype(jnp.float32), w_uk.astype(jnp.float32), w_uv.astype(jnp.float32), w_o.astype(jnp.float32))
    cotangents = pullback(y_grad.astype(jnp.float32))
    return (y_full.astype(jnp.bfloat16), cotangents[0].astype(jnp.bfloat16), cotangents[1], cotangents[2], cotangents[3], cotangents[4], cotangents[5], cotangents[6], cotangents[7])
```

```python
import functools

import jax
import jax.numpy as jnp
from jax import lax
from jax.experimental import pallas as pl
from jax.experimental.pallas import tpu as pltpu
from jax.sharding import PartitionSpec as P


ROPE_THETA = 10000.0
NORM_EPS = 1e-6
LOG2E = 1.4426950408889634
MASKED = -1e30
F32 = jnp.float32
BF16 = jnp.bfloat16
OVER_ROWS = (((0,), (0,)), ((), ()))
OVER_COLS = (((1,), (1,)), ((), ()))
LANES = 128
SLOT = 2 * LANES
VMEM_LIMIT = 63 * 1024 * 1024
EVENTS = 36


def compiler_params(**more):
    return pltpu.CompilerParams(vmem_limit_bytes=VMEM_LIMIT, **more)


def cost(flops, bytes_accessed=0, transcendentals=0):
    return pl.CostEstimate(flops=int(flops), bytes_accessed=bytes_accessed, transcendentals=transcendentals)


def struct(shape, dtype=F32):
    return jax.ShapeDtypeStruct(shape, dtype)


def whole(*shape):
    return pl.BlockSpec(shape, lambda *i: (0,) * len(shape))


def rows(count, width):
    return pl.BlockSpec((count, width), lambda i, *_: (i, 0))


def zero(*refs):
    for ref in refs:
        ref[...] = jnp.zeros(ref.shape, ref.dtype)


def exact(a, b):
    return jnp.dot(a, b, preferred_element_type=F32)


def over_rows(a, b):
    return lax.dot_general(a, b, OVER_ROWS, preferred_element_type=F32)


def at_block(index, size):
    return pl.ds(pl.multiple_of(index * size, size), size)


def rope_tables(positions, rope_dim):
    half_dim = rope_dim // 2
    inv_freq = ROPE_THETA ** (-(jnp.arange(half_dim, dtype=F32) * 2.0 / rope_dim))
    angles = positions.astype(F32)[:, None] * inv_freq[None, :]
    return jnp.cos(angles), jnp.sin(angles)


def rope_back(g_in, cos_t, sin_t):
    first_half, second_half = jnp.split(g_in, 2, axis=-1)
    return jnp.concatenate([first_half * cos_t + second_half * sin_t, second_half * cos_t - first_half * sin_t], axis=-1)


def attn_kernel(scale, shard, half, nope, rope, core_ref, x_ref, far_ref, near_ref, w_ref, wt_ref, gain_ref, wkv_ref, g_ref,
                odq_ref, keep_ref, give_ref, latent_ref,
                w2_ref, q_ref, k_ref, v_ref, kt_ref, vt_ref, cm_ref, sm_ref, s_ref, m_ref, l_ref, do_ref, d_ref, acc_ref, dk_ref, dv_ref):
    i = pl.program_id(0)
    n = pl.num_programs(0)
    core = core_ref[0]
    bq = q_ref.shape[0]
    bk = x_ref.shape[0]
    vd = v_ref.shape[1]
    rep = bk // LANES

    def keys(j):
        return at_block(j, bk)

    def wide(x):
        return jnp.concatenate([x] * rep, axis=1)

    def fold(x, op):
        return functools.reduce(op, jnp.split(x, rep, axis=1))

    def swapped(t):
        lane = lax.broadcasted_iota(jnp.int32, t.shape, 1)
        return jnp.where(lane % rope < rope // 2, pltpu.roll(t, LANES - rope // 2, 1), pltpu.roll(t, rope // 2, 1))

    def spread(ref, column):
        ref[...] = jnp.broadcast_to(column, ref.shape)

    @pl.when(i == 0)
    def _():
        w2_ref[...] = wt_ref[...].T
        zero(dk_ref, dv_ref)

    step = near_ref.shape[0]

    def project(b, _):
        r = at_block(b, step)
        t = at_block(i * (bk // step) + b, step)
        x = x_ref[r, :]
        c = exact(x, w_ref[...])
        inv = lax.rsqrt(jnp.sum(c * c, axis=1, keepdims=True) * (1.0 / c.shape[1]) + NORM_EPS)
        latent = (c * inv * gain_ref[...]).astype(BF16)
        latent_ref[r, :] = latent
        kv = exact(latent, wkv_ref[...])
        v_ref[t, :] = kv[:, nope:].astype(BF16)
        qk = exact(x, w2_ref[...])
        far = far_ref[pl.ds(i * (bk // step) + b, 1), :]
        lane = lax.broadcasted_iota(jnp.int32, (step, LANES), 1)
        cos_a, sin_a = far[:, :LANES], far[:, LANES:]
        cos_b, sin_b = near_ref[:, :LANES], near_ref[:, LANES:]
        cos_t = cos_a * cos_b - sin_a * sin_b
        sin_t = sin_a * cos_b + cos_a * sin_b
        sin_t = jnp.where(lane % rope < rope // 2, -sin_t, sin_t)
        turned = qk[:, nope:]
        turned = turned * cos_t + swapped(turned) * sin_t
        k = jnp.concatenate([kv[:, :nope], jnp.where(lane < rope, pltpu.roll(turned, rope, 1), 0.0)], axis=1).astype(BF16)
        k_ref[t, :] = k
        kt_ref[:, t] = k.T
        vt_ref[:, t] = kv[:, nope:].astype(BF16).T
        q = jnp.concatenate([qk[:, :nope], jnp.where(lane < rope, turned, 0.0)], axis=1).astype(BF16)
        for a in range(step // shard):
            to = at_block(b * (step // shard) + a, half)
            lo, hi = slice(a * shard, a * shard + half), slice(a * shard + half, (a + 1) * shard)
            for ref, value in ((q_ref, q), (cm_ref, cos_t), (sm_ref, sin_t)):
                ref[to, :] = jnp.where(core == 0, value[lo], value[hi])
        return 0

    lax.fori_loop(0, bk // step, project, 0)

    m_ref[...] = jnp.full(m_ref.shape, MASKED, F32)

    def scores(j):
        return exact(q_ref[...], kt_ref[:, keys(j)])

    def note(j, s):
        s_ref[:, keys(j)] = s
        m_ref[...] = jnp.maximum(m_ref[...], fold(s, jnp.maximum))

    def full_tile(j, _):
        note(j, scores(j))
        return 0

    lax.fori_loop(0, i, full_tile, 0)
    row = lax.broadcasted_iota(jnp.int32, (bq, bk), 0)
    col = lax.broadcasted_iota(jnp.int32, (bq, bk), 1)
    note(i, jnp.where(col <= (row // half) * shard + core * half + row % half, scores(i), MASKED))

    spread(m_ref, jnp.max(m_ref[...], axis=1, keepdims=True))
    zero(l_ref, acc_ref)

    def prob_tile(j, _):
        r = keys(j)
        p = jnp.exp2((s_ref[:, r] - wide(m_ref[...])) * (scale * LOG2E))
        s_ref[:, r] = p
        l_ref[...] += fold(p, jnp.add)
        acc_ref[:, :vd] += exact(p.astype(BF16), v_ref[r, :])
        return 0

    lax.fori_loop(0, i + 1, prob_tile, 0)

    inv = 1.0 / jnp.sum(l_ref[...], axis=1, keepdims=True)
    o = acc_ref[:, :vd] * inv
    odq_ref[:, :vd] = o.astype(BF16)
    do = g_ref[...].astype(F32)
    spread(d_ref, jnp.sum(do * o, axis=1, keepdims=True) * inv)
    do_ref[...] = (do * inv).astype(BF16)
    zero(acc_ref)

    def back_tile(j, _):
        r = keys(j)
        p = s_ref[:, r]
        dp = exact(do_ref[...], vt_ref[:, r])
        ds = (p * (dp - wide(d_ref[...]))).astype(BF16)
        dv_ref[r, :] += over_rows(p.astype(BF16), do_ref[...])
        dk_ref[r, :] += over_rows(ds, q_ref[...])
        acc_ref[...] += exact(ds, k_ref[r, :])
        return 0

    lax.fori_loop(0, i + 1, back_tile, 0)
    dq = acc_ref[...] * scale
    turned = dq[:, nope:]
    turned = turned * cm_ref[...] - swapped(turned) * sm_ref[...]
    odq_ref[:, vd:vd + nope] = dq[:, :nope].astype(BF16)
    odq_ref[:, vd + nope:] = turned.astype(BF16)

    @pl.when(i == n - 1)
    def _():
        def finish(s, _):
            to = at_block(s, half)
            for ref, side in ((keep_ref, core), (give_ref, 1 - core)):
                r = at_block(2 * s + side, half)
                ref[to, :SLOT] = dk_ref[r, :] * scale
                ref[to, SLOT:] = dv_ref[r, :]
            return 0

        lax.fori_loop(0, dk_ref.shape[0] // shard, finish, 0)


def attention(core, x, far, near, w_dkv, wt, gain, wkv, g, scale, shard, nope, rope, n):
    seq, d_model = x.shape
    rank, vd = w_dkv.shape[1], g.shape[1]
    half, nq, bk = shard // 2, seq // 2, seq // n
    bq = nq // n
    vmem = lambda *shape: pltpu.VMEM(shape, F32)
    packed = lambda *shape: pltpu.VMEM(shape, BF16)
    return pl.pallas_call(
        functools.partial(attn_kernel, scale, shard, half, nope, rope),
        grid_spec=pltpu.PrefetchScalarGridSpec(
            num_scalar_prefetch=1, grid=(n,),
            in_specs=[rows(bk, d_model), whole(*far.shape), whole(*near.shape), whole(*w_dkv.shape), whole(*wt.shape), whole(*gain.shape), whole(*wkv.shape), rows(bq, vd)],
            out_specs=[rows(bq, vd + SLOT), whole(nq, SLOT + vd), whole(nq, SLOT + vd), rows(bk, rank)],
            scratch_shapes=[packed(d_model, SLOT), packed(bq, SLOT), packed(seq, SLOT), packed(seq, vd), packed(SLOT, seq), packed(vd, seq),
                            vmem(bq, LANES), vmem(bq, LANES), vmem(bq, seq), vmem(bq, LANES), vmem(bq, LANES), packed(bq, vd), vmem(bq, LANES), vmem(bq, SLOT),
                            vmem(seq, SLOT), vmem(seq, vd)]),
        out_shape=[struct((nq, vd + SLOT), BF16), struct((nq, SLOT + vd)), struct((nq, SLOT + vd)), struct((seq, rank), BF16)],
        compiler_params=compiler_params(),
        cost_estimate=cost(2 * seq * d_model * (rank + SLOT) + 7 * nq * seq * SLOT, 2 * x.size, nq * seq),
    )(core[None], x, far, near, w_dkv, wt, gain, wkv, g)


def ring_kernel(side, counts, make, n_given, n_made, *refs):
    n_ring, n_each, n_same = counts
    total = sum(counts)
    given = refs[:n_given]
    srcs, outs = refs[n_given:n_given + total - n_made], refs[n_given + total - n_made:n_given + 2 * total - n_made]
    send_sem, recv_sem, own_sem, *rest = refs[n_given + 2 * total - n_made:]
    direct_sem, made = rest[:2], rest[2:]
    srcs = [*srcs, *made[:n_made]]
    n_dev = 2 * side * side
    me = lax.axis_index("cp")
    pos = ((me // 2) % side, me // (2 * side))
    mesh_id = pl.DeviceIdType.MESH

    def at(dx, dy):
        return (lax.rem(pos[1] + dy + side, side) * side + lax.rem(pos[0] + dx + side, side)) * 2 + me % 2

    def shifted(color, first, second):
        return at(second, first) if color else at(first, second)

    sibling = me + 1 - 2 * (me % 2)
    direct = n_each + n_same > 0
    neighbours = [shifted(color, d, 0) for color in range(2) for d in (1, -1)]
    peers = [me ^ d for d in range(1, n_dev)] if direct else [*neighbours, sibling]
    barrier = pltpu.get_barrier_semaphore()
    for peer in peers:
        pl.semaphore_signal(barrier, inc=1, device_id={"cp": peer}, device_id_type=mesh_id)
    pl.semaphore_wait(barrier, len(peers))

    def part(ref, color, piece=0, pieces=1):
        size = ref.shape[0] // (2 * pieces)
        return ref.at[pl.ds((pieces * color + piece) * size, size)]

    def copy(src, dst, sems, peer):
        return pltpu.make_async_remote_copy(src_ref=src, dst_ref=dst, send_sem=sems[0], recv_sem=sems[1], device_id={"cp": peer}, device_id_type=mesh_id)

    def sems(k, color, event):
        return send_sem.at[k, color, event], recv_sem.at[k, color, event]

    pending = []

    def send(color, event, block, peer, *piece):
        for k in range(n_ring):
            src, dst = (srcs[k], outs[k].at[me]) if block is None else (outs[k].at[block],) * 2
            pending.append(copy(part(src, color, *piece), part(dst, color, *piece), sems(k, color, event), peer))
            pending[-1].start()

    def arrived(color, event, block, *piece):
        for k in range(n_ring):
            ref = part(outs[k].at[block], color, *piece)
            copy(ref, ref, sems(k, color, event), sibling).wait_recv()

    own = [pltpu.make_async_copy(srcs[k].at[me] if n_ring <= k < n_ring + n_each else srcs[k], outs[k].at[me], own_sem.at[k]) for k in range(total)]
    straight = []
    for k in range(n_ring, total):
        for d in range(1, n_dev):
            peer = me ^ d
            src = srcs[k].at[peer] if k < n_ring + n_each else srcs[k]
            straight.append(copy(src, outs[k].at[me], [s.at[k - n_ring, d] for s in direct_sem], peer))
    late = own[n_ring:] + straight
    if not make:
        late, early = [], own + straight
    else:
        early = own[:n_ring]
    for c in early:
        c.start()
    finish = make(*given, *made) if make else None

    colors = range(2)
    offsets = (0, -1, 1, 2)
    first_out, relays, second_out, to_sibling, column = 0, 2, 4, 20, 24

    def spread(c, j, block):
        for d, way in enumerate((1, -1)):
            send(c, second_out + 4 * j + d, block, shifted(c, 0, way))
        send(c, to_sibling + j, block, sibling)

    def relay(c, j):
        for d, way in enumerate((1, -1)):
            block = shifted(c, offsets[j], -way)
            arrived(c, second_out + 4 * j + d, block)
            send(c, second_out + relays + 4 * j + d, block, shifted(c, 0, way), d, 2)
            send(c, column + 3 * j + d, block, sibling)

    if not n_ring:
        for c in own + straight:
            c.wait()
        return
    for c in colors:
        for d, way in enumerate((1, -1)):
            send(c, first_out + d, None, shifted(c, way, 0))
        spread(c, 0, None)
    if make:
        finish()
    for c in colors:
        for d, way in enumerate((1, -1)):
            block = shifted(c, -way, 0)
            arrived(c, first_out + d, block)
            send(c, relays + d, block, shifted(c, way, 0), d, 2)
            spread(c, 1 + d, block)
    for c in late:
        c.start()
    for c in colors:
        relay(c, 0)
    for c in colors:
        across = shifted(c, 2, 0)
        for d in range(2):
            arrived(c, relays + d, across, d, 2)
        spread(c, 3, across)
    for j in range(1, 4):
        for c in colors:
            relay(c, j)
    for j in range(4):
        for c in colors:
            across = shifted(c, offsets[j], 2)
            for d in range(2):
                arrived(c, second_out + relays + 4 * j + d, across, d, 2)
            send(c, column + 2 + 3 * j, across, sibling)
    other = sibling - me
    for c in colors:
        for j in range(4):
            arrived(c, to_sibling + j, shifted(c, offsets[j], 0) + other)
            for d in range(3):
                arrived(c, column + 3 * j + d, shifted(c, offsets[j], offsets[1 + d]) + other)
    for c in pending:
        c.wait_send()
    for c in own + straight:
        c.wait()


def ring_gather(n_dev, cid, ring, each=(), same=(), make=None, given=(), scratch=()):
    side = round((n_dev // 2) ** 0.5)
    sent = [*ring, *each, *same]
    n_made = 1 if make else 0
    shapes = [struct(a.shape if len(ring) <= k < len(ring) + len(each) else (n_dev,) + a.shape, a.dtype) for k, a in enumerate(sent)]
    shapes += [struct(a.shape, a.dtype) for a in scratch[:n_made]]
    counts = len(ring), len(each) + n_made, len(same)
    n_direct = sum(counts[1:])
    dma = pltpu.SemaphoreType.DMA
    in_vmem, anywhere = pl.BlockSpec(memory_space=pltpu.VMEM), pl.BlockSpec(memory_space=pl.ANY)
    return pl.pallas_call(
        functools.partial(ring_kernel, side, counts, make, len(given), n_made),
        in_specs=[anywhere] * len(given) + [in_vmem] * len(sent), out_specs=[anywhere] * len(shapes), out_shape=shapes,
        scratch_shapes=[dma((max(len(ring), 1), 2, EVENTS))] * 2 + [dma((len(shapes),))] + [dma((max(n_direct, 1), n_dev))] * 2 + list(scratch),
        compiler_params=compiler_params(collective_id=cid, has_side_effects=True),
        cost_estimate=cost(4e10),
    )(*given, *sent)


def make_d_out(gy_ref, w_ref, blocks_ref, gy_vmem, w_vmem, sems):
    reads = [pltpu.make_async_copy(src, dst, sems.at[k]) for k, (src, dst) in enumerate(((gy_ref, gy_vmem), (w_ref, w_vmem)))]
    for c in reads:
        c.start()

    def compute():
        for c in reads:
            c.wait()
        heads, v_dim = w_ref.shape[:2]
        half = blocks_ref.shape[1]

        def two_heads(b, _):
            w = w_vmem[pl.ds(2 * b, 2)].reshape(2 * v_dim, -1)
            g = lax.dot_general(gy_vmem[...], w, OVER_COLS, preferred_element_type=F32).astype(BF16)
            for h in range(2):
                for core in range(2):
                    blocks_ref[4 * b + 2 * h + core] = g[core * half:(core + 1) * half, h * v_dim:(h + 1) * v_dim]
            return 0

        lax.fori_loop(0, heads // 2, two_heads, 0)

    return compute


def query_grads_kernel(qk_dim, core_ref, x_ref, odq_ref, keep_ref, give_ref, q_acc):
    i = pl.program_id(0)
    core = core_ref[0]
    d_model = x_ref.shape[-1]

    @pl.when(i == 0)
    def _():
        zero(q_acc)

    x = x_ref[...].reshape(-1, d_model)
    dq_t = odq_ref[...].T[-SLOT:][:qk_dim]
    for c in range(4):
        cols = slice(c * d_model // 4, (c + 1) * d_model // 4)
        q_acc[:, cols] += exact(dq_t, x[:, cols])

    @pl.when(i == pl.num_programs(0) - 1)
    def _():
        for ref, side in ((keep_ref, core), (give_ref, 1 - core)):
            ref[...] = q_acc[at_block(side, qk_dim // 2), :]


def output_grads_kernel(core_ref, gy_ref, odq_ref, keep_ref, give_ref, o_acc):
    i = pl.program_id(0)
    core = core_ref[0]
    vd, d_model = o_acc.shape

    @pl.when(i == 0)
    def _():
        zero(o_acc)

    gy = gy_ref[...].reshape(-1, d_model)
    o_t = odq_ref[...].T[:vd]
    for c in range(4):
        cols = slice(c * d_model // 4, (c + 1) * d_model // 4)
        o_acc[:, cols] += exact(o_t, gy[:, cols])

    @pl.when(i == pl.num_programs(0) - 1)
    def _():
        for ref, side in ((keep_ref, core), (give_ref, 1 - core)):
            ref[...] = o_acc[at_block(side, vd // 2), :]


def head_grads(kernel, core, act, odq, n_dev, half, width):
    n = 4
    shards = n_dev // n
    d_model = act.shape[1]
    out = width // 2, d_model
    return pl.pallas_call(
        kernel,
        grid_spec=pltpu.PrefetchScalarGridSpec(
            num_scalar_prefetch=1, grid=(n,),
            in_specs=[pl.BlockSpec((shards, 1, half, d_model), lambda i, c: (i, c[0], 0, 0)), rows(shards * half, odq.shape[1])],
            out_specs=[whole(*out)] * 2, scratch_shapes=[pltpu.VMEM((width, d_model), F32)]),
        out_shape=[struct(out)] * 2, compiler_params=compiler_params(), cost_estimate=cost(act.size * width, act.size),
    )(core[None], act.reshape(n_dev, 2, half, d_model), odq)


def up_grads_kernel(core_ref, latent_ref, kv_ref, keep_ref, give_ref):
    core = core_ref[0]
    up = over_rows(latent_ref[...].reshape(-1, latent_ref.shape[-1]), kv_ref[...])
    count = keep_ref.shape[0]
    width = up.shape[1]
    blocks = keep_ref.shape[1] // width
    for a in range(blocks):
        lo, hi = (up[(s * blocks + a) * count:(s * blocks + a + 1) * count] for s in range(2))
        cols = slice(a * width, (a + 1) * width)
        keep_ref[:, cols] = jnp.where(core == 0, lo, hi)
        give_ref[:, cols] = jnp.where(core == 0, hi, lo)


def up_grads(core, latent, kv, d_model, n_dev, half):
    rank, width = latent.shape[1], kv.shape[1]
    out = rank * width // (2 * d_model), d_model
    return pl.pallas_call(
        up_grads_kernel,
        grid_spec=pltpu.PrefetchScalarGridSpec(
            num_scalar_prefetch=1, grid=(1,),
            in_specs=[pl.BlockSpec((n_dev, 1, half, rank), lambda i, c: (0, c[0], 0, 0)), whole(*kv.shape)], out_specs=[whole(*out)] * 2),
        out_shape=[struct(out)] * 2, compiler_params=compiler_params(), cost_estimate=cost(2 * kv.size * rank, latent.size),
    )(core[None], latent.reshape(n_dev, 2, half, rank), kv)


def low_grads_kernel(x_ref, low_ref, dkv_ref, kr_ref, low_t):
    @pl.when(pl.program_id(0) == 0)
    def _():
        count = low_ref.shape[0] // 8

        def turn(b, _):
            r = at_block(b, count)
            low_t[:, r] = low_ref[r, :].T
            return 0

        lax.fori_loop(0, 8, turn, 0)

    g = exact(low_t[...], x_ref[...])
    rank = dkv_ref.shape[1]
    dkv_ref[...] = g[:rank].T
    kr_ref[...] = g[rank:]


def low_grads(x, low, rank, rope):
    seq, d_model = x.shape
    return pl.pallas_call(
        low_grads_kernel, grid=(d_model // SLOT,),
        in_specs=[pl.BlockSpec((seq, SLOT), lambda i: (0, i)), whole(*low.shape)],
        out_specs=[rows(SLOT, rank), pl.BlockSpec((rope, SLOT), lambda i: (0, i))],
        out_shape=[struct((d_model, rank)), struct((rope, d_model))],
        scratch_shapes=[pltpu.VMEM(low.shape[::-1], BF16)],
        compiler_params=compiler_params(), cost_estimate=cost(2 * x.size * (rank + rope), 2 * x.size),
    )(x, low)


def copy_kernel(src_ref, dst_ref):
    dst_ref[...] = src_ref[...]


def copied(a):
    block = rows(a.shape[0] // 8, a.shape[1])
    return pl.pallas_call(copy_kernel, grid=(8,), in_specs=[block], out_specs=block, out_shape=struct(a.shape, a.dtype),
                          compiler_params=compiler_params(), cost_estimate=cost(1e9, 8 * a.size))(a)


def spread_heads_kernel(up_ref, uk_ref, uv_ref):
    heads, _, count, cols = up_ref.shape
    for a, block in enumerate(jnp.split(up_ref[...].reshape(heads, count, cols), cols // SLOT, axis=2)):
        for ref, value in zip((uk_ref, uv_ref), jnp.split(block, 2, axis=2)):
            ref[a * count:(a + 1) * count] = jnp.swapaxes(value, 0, 1)


def spread_heads(up, rank, width):
    heads, _, count, cols = up.shape
    steps = 2
    return pl.pallas_call(
        spread_heads_kernel, grid=(2, steps),
        in_specs=[pl.BlockSpec((heads, 1, count, cols // steps), lambda s, a: (0, s, 0, a))],
        out_specs=[pl.BlockSpec((rank // (2 * steps), heads, width), lambda s, a: (s * steps + a, 0, 0))] * 2,
        out_shape=[struct((rank, heads, width))] * 2, compiler_params=compiler_params(), cost_estimate=cost(1e9, 8 * up.size),
    )(up)


def solution(mesh):
    n_dev = mesh.shape['cp']
    row_spec, per_group = P(('dp', 'cp')), P('dp')
    siblings = [(i, i ^ 1) for i in range(n_dev)]

    def block(x_loc, gy_loc, w_q, w_dkv, g_kv, w_kr, w_uk, w_uv, w_o):
        shard, d_model = x_loc.shape
        heads, qk_dim = w_q.shape[1:]
        rank, _, nope = w_uk.shape
        v_dim, rope = w_uv.shape[2], w_kr.shape[1]
        half, seq = shard // 2, n_dev * shard
        me = lax.axis_index('cp')
        head, core = me // 2, me % 2

        def gather(a):
            return lax.all_gather(a, 'cp', axis=0, tiled=True)

        def summed(keep, give):
            return keep + lax.ppermute(give, 'cp', siblings)

        packed = lambda *shape: pltpu.VMEM(shape, BF16)
        scratch = packed(n_dev, half, v_dim), packed(*gy_loc.shape), packed(*w_o.shape), pltpu.SemaphoreType.DMA((2,))
        x_all, d_out = ring_gather(n_dev, 1, [x_loc], make=make_d_out, given=[gy_loc, w_o], scratch=scratch)
        x_all, d_out = x_all.reshape(seq, d_model), d_out.reshape(seq // 2, v_dim)
        gy_all = gather(lax.optimization_barrier((gy_loc, x_all))[0])

        pick = lambda a, axis: lax.dynamic_index_in_dim(a, head, axis, False)
        wt = jnp.concatenate([pick(w_q.transpose(1, 2, 0), 0), w_kr.T], axis=0)
        wkv = jnp.concatenate([pick(w_uk, 1), pick(w_uv, 1)], axis=1)
        w_uk, w_uv, _ = lax.optimization_barrier((w_uk, w_uv, x_all))

        def table(positions):
            return jnp.concatenate([t for t in rope_tables(positions, rope) for _ in range(4)], axis=1)

        far, near = table(jnp.arange(0, seq, 4 * shard)), table(jnp.arange(4 * shard))
        gain = g_kv.astype(F32)[None]
        odq, kv_keep, kv_give, latent = attention(core, x_all, far, near, w_dkv, wt, gain, wkv, d_out, qk_dim ** -0.5, shard, nope, rope, 4)

        q_keep, q_give = head_grads(functools.partial(query_grads_kernel, qk_dim), core, x_all, odq, n_dev, half, qk_dim)
        gwq = gather(summed(q_keep, q_give))

        kv_sum = lax.optimization_barrier((summed(kv_keep, kv_give), q_keep))[0]
        kv_my = jnp.concatenate([kv_sum[:, :nope], kv_sum[:, SLOT:]], axis=1).astype(BF16)
        dkr_my = kv_sum[:, nope:qk_dim].reshape(n_dev, half * rope // LANES, LANES)
        got = lax.all_to_all(jnp.concatenate([odq, kv_my], axis=1).reshape(n_dev, half, -1), 'cp', 0, 0, tiled=True)
        o_keep, o_give = head_grads(output_grads_kernel, core, gy_all, odq, n_dev, half, v_dim)
        o_my = summed(o_keep, o_give)
        gwo = gather(o_my)
        up_keep, up_give = up_grads(core, latent, kv_my, d_model, n_dev, half)
        up_my = summed(up_keep, up_give)
        got_r, = ring_gather(n_dev, 2, [], [lax.optimization_barrier((dkr_my, o_my, up_my))[0]])

        got, got_r = lax.optimization_barrier((got, got_r))
        dkr_loc = jnp.sum(got_r.reshape(heads, shard, rope), axis=0)
        got = got.reshape(heads, shard, -1)
        o_loc, dq_loc, _, dk_loc, dv_loc = jnp.split(got, [v_dim, v_dim + qk_dim, v_dim + SLOT, v_dim + SLOT + nope], axis=2)
        y_loc = jnp.einsum('htv,hvd->td', o_loc, w_o, preferred_element_type=F32).astype(BF16)
        d_latent = jnp.einsum('htn,chn->tc', dk_loc, w_uk, preferred_element_type=F32) + jnp.einsum('htv,chv->tc', dv_loc, w_uv, preferred_element_type=F32)
        c_loc = exact(x_loc, w_dkv)
        inv_loc = lax.rsqrt(jnp.mean(c_loc * c_loc, axis=-1, keepdims=True) + NORM_EPS)
        c_norm = c_loc * inv_loc
        gg_part = jnp.sum(d_latent * c_norm, axis=0)
        d_norm = d_latent * gain
        dc_loc = (inv_loc * (d_norm - c_norm * jnp.mean(d_norm * c_norm, axis=-1, keepdims=True))).astype(BF16)
        cos_t, sin_t = rope_tables(me * shard + jnp.arange(shard), rope)
        dkr_raw = rope_back(dkr_loc, cos_t, sin_t).astype(BF16)
        dx_loc = jnp.einsum('hte,dhe->td', dq_loc, w_q, preferred_element_type=F32) + jnp.einsum('tc,dc->td', dc_loc, w_dkv, preferred_element_type=F32) + jnp.einsum('tr,dr->td', dkr_raw, w_kr, preferred_element_type=F32)

        gg_rows = rank // LANES
        gg_part = jnp.pad(gg_part.reshape(gg_rows, LANES), ((0, 8 - gg_rows), (0, 0)))
        low, up, gg = ring_gather(n_dev, 3, [jnp.concatenate([dc_loc, dkr_raw], axis=1), up_my], (), [gg_part])
        gw_dkv, gw_kr = low_grads(x_all, low.reshape(seq, rank + rope), rank, rope)
        gg_kv = jnp.sum(gg, axis=0)[:gg_rows].reshape(rank)
        gwq = copied(gwq)
        gw_uk, gw_uv = spread_heads(up.reshape(heads, 2, -1, d_model), rank, nope)
        gw_q = gwq.reshape(heads, qk_dim, d_model).transpose(2, 0, 1)
        return y_loc, dx_loc.astype(BF16), gw_q, gw_dkv, gg_kv, gw_kr.T, gw_uk, gw_uv, gwo.reshape(heads, v_dim, d_model)

    return jax.shard_map(block, mesh=mesh, in_specs=(row_spec, row_spec) + (P(),) * 7, out_specs=(row_spec, row_spec) + (per_group,) * 7, check_vma=False)
```

```python
import functools

import jax
import jax.numpy as jnp
import numpy as np
from jax import lax
from jax.experimental import pallas as pl
from jax.experimental.pallas import tpu as pltpu
from jax.sharding import PartitionSpec as P


ROPE_THETA = 10000.0
NORM_EPS = 1e-6
LOG2E = 1.4426950408889634
MASKED = -1e30
F32 = jnp.float32
BF16 = jnp.bfloat16
OVER_ROWS = (((0,), (0,)), ((), ()))
OVER_COLS = (((1,), (1,)), ((), ()))
LANES = 128
SLOT = 2 * LANES
VMEM_LIMIT = 63 * 1024 * 1024
EVENTS = 36


def compiler_params(**more):
    return pltpu.CompilerParams(vmem_limit_bytes=VMEM_LIMIT, **more)


def cost(flops, bytes_accessed=0, transcendentals=0):
    return pl.CostEstimate(flops=int(flops), bytes_accessed=bytes_accessed, transcendentals=transcendentals)


def struct(shape, dtype=F32):
    return jax.ShapeDtypeStruct(shape, dtype)


def whole(*shape):
    return pl.BlockSpec(shape, lambda *i: (0,) * len(shape))


def rows(count, width):
    return pl.BlockSpec((count, width), lambda i, *_: (i, 0))


def zero(*refs):
    for ref in refs:
        ref[...] = jnp.zeros(ref.shape, ref.dtype)


def exact(a, b):
    return jnp.dot(a, b, preferred_element_type=F32)


def over_rows(a, b):
    return lax.dot_general(a, b, OVER_ROWS, preferred_element_type=F32)


def over_cols(a, b):
    return lax.dot_general(a, b, OVER_COLS, preferred_element_type=F32)


def at_block(index, size):
    return pl.ds(pl.multiple_of(index * size, size), size)


def rope_tables(positions, rope_dim, xp=jnp):
    half_dim = rope_dim // 2
    inv_freq = ROPE_THETA ** (-(xp.arange(half_dim, dtype=xp.float32) * 2.0 / rope_dim))
    angles = positions[:, None] * inv_freq[None, :]
    return xp.cos(angles), xp.sin(angles)


def rope_back(g_in, cos_t, sin_t):
    first_half, second_half = jnp.split(g_in, 2, axis=-1)
    return jnp.concatenate([first_half * cos_t + second_half * sin_t, second_half * cos_t - first_half * sin_t], axis=-1)


def attn_kernel(scale, shard, half, nope, rope, place_ref, x_ref, far_ref, near_ref, w_ref, wq_ref, wr_ref, gain_ref, uk_ref, uv_ref, g_ref,
                odq_ref, keep_ref, give_ref, latent_ref,
                w2_ref, wkv_ref, q_ref, k_ref, v_ref, cm_ref, sm_ref, s_ref, m_ref, l_ref, do_ref, d_ref, acc_ref, dk_ref, dv_ref):
    i = pl.program_id(0)
    n = pl.num_programs(0)
    core = place_ref[0]
    bq = q_ref.shape[0]
    bk = x_ref.shape[0]
    vd = v_ref.shape[1]
    rep = bk // LANES

    def keys(j):
        return at_block(j, bk)

    def wide(x):
        return jnp.concatenate([x] * rep, axis=1)

    def fold(x, op):
        return functools.reduce(op, jnp.split(x, rep, axis=1))

    def swapped(t):
        lane = lax.broadcasted_iota(jnp.int32, t.shape, 1)
        return jnp.where(lane % rope < rope // 2, pltpu.roll(t, LANES - rope // 2, 1), pltpu.roll(t, rope // 2, 1))

    def both_tables(t):
        first = lax.broadcasted_iota(jnp.int32, t.shape, 1) < rope
        other = pltpu.roll(t, rope, 1)
        return jnp.where(first, t, other), jnp.where(first, other, t)

    def spread(ref, column):
        ref[...] = jnp.broadcast_to(column, ref.shape)

    @pl.when(i == 0)
    def _():
        w2_ref[...] = jnp.concatenate([wq_ref[0], wr_ref[...]], axis=0).T
        wkv_ref[:, :nope] = uk_ref[...]
        wkv_ref[:, nope:] = uv_ref[...]
        zero(dk_ref, dv_ref)

    step = near_ref.shape[0]

    def project(b, _):
        r = at_block(b, step)
        t = at_block(i * (bk // step) + b, step)
        x = x_ref[r, :]
        c = exact(x, w_ref[...])
        inv = lax.rsqrt(jnp.sum(c * c, axis=1, keepdims=True) * (1.0 / c.shape[1]) + NORM_EPS)
        latent = (c * inv * gain_ref[...]).astype(BF16)
        latent_ref[r, :] = latent
        kv = exact(latent, wkv_ref[...])
        v_ref[t, :] = kv[:, nope:].astype(BF16)
        qk = exact(x, w2_ref[...])
        far = far_ref[pl.ds(i * (bk // step) + b, 1), :]
        lane = lax.broadcasted_iota(jnp.int32, (step, LANES), 1)
        (cos_a, sin_a), (cos_b, sin_b) = both_tables(far), both_tables(near_ref[...])
        cos_t = cos_a * cos_b - sin_a * sin_b
        sin_t = sin_a * cos_b + cos_a * sin_b
        sin_t = jnp.where(lane % rope < rope // 2, -sin_t, sin_t)
        turned = qk[:, nope:]
        turned = turned * cos_t + swapped(turned) * sin_t
        k_ref[t, :] = jnp.concatenate([kv[:, :nope], jnp.where(lane < rope, pltpu.roll(turned, rope, 1), 0.0)], axis=1).astype(BF16)
        q = jnp.concatenate([qk[:, :nope], jnp.where(lane < rope, turned, 0.0)], axis=1).astype(BF16)
        for a in range(step // shard):
            to = at_block(b * (step // shard) + a, half)
            lo, hi = slice(a * shard, a * shard + half), slice(a * shard + half, (a + 1) * shard)
            for ref, value in ((q_ref, q), (cm_ref, cos_t), (sm_ref, sin_t)):
                ref[to, :] = jnp.where(core == 0, value[lo], value[hi])
        return 0

    lax.fori_loop(0, bk // step, project, 0)

    m_ref[...] = jnp.full(m_ref.shape, MASKED, F32)

    def scores(j):
        return over_cols(q_ref[...], k_ref[keys(j), :])

    def note(j, s):
        s_ref[:, keys(j)] = s
        m_ref[...] = jnp.maximum(m_ref[...], fold(s, jnp.maximum))

    def full_tile(j, _):
        note(j, scores(j))
        return 0

    lax.fori_loop(0, i, full_tile, 0)
    row = lax.broadcasted_iota(jnp.int32, (bq, bk), 0)
    col = lax.broadcasted_iota(jnp.int32, (bq, bk), 1)
    note(i, jnp.where(col <= (row // half) * shard + core * half + row % half, scores(i), MASKED))

    spread(m_ref, jnp.max(m_ref[...], axis=1, keepdims=True))
    zero(l_ref, acc_ref)

    def prob_tile(j, _):
        r = keys(j)
        p = jnp.exp2((s_ref[:, r] - wide(m_ref[...])) * (scale * LOG2E))
        s_ref[:, r] = p
        l_ref[...] += fold(p, jnp.add)
        acc_ref[:, :vd] += exact(p.astype(BF16), v_ref[r, :])
        return 0

    lax.fori_loop(0, i + 1, prob_tile, 0)

    inv = 1.0 / jnp.sum(l_ref[...], axis=1, keepdims=True)
    o = acc_ref[:, :vd] * inv
    odq_ref[:, :vd] = o.astype(BF16)
    do = g_ref[...].astype(F32)
    spread(d_ref, jnp.sum(do * o, axis=1, keepdims=True) * inv)
    do_ref[...] = (do * inv).astype(BF16)
    zero(acc_ref)

    def back_tile(j, _):
        r = keys(j)
        p = s_ref[:, r]
        dp = over_cols(do_ref[...], v_ref[r, :])
        ds = (p * (dp - wide(d_ref[...]))).astype(BF16)
        dv_ref[r, :] += over_rows(p.astype(BF16), do_ref[...])
        dk_ref[r, :] += over_rows(ds, q_ref[...])
        acc_ref[...] += exact(ds, k_ref[r, :])
        return 0

    lax.fori_loop(0, i + 1, back_tile, 0)
    dq = acc_ref[...] * scale
    turned = dq[:, nope:]
    turned = turned * cm_ref[...] - swapped(turned) * sm_ref[...]
    odq_ref[:, vd:vd + nope] = dq[:, :nope].astype(BF16)
    odq_ref[:, vd + nope:] = turned.astype(BF16)

    @pl.when(i == n - 1)
    def _():
        def finish(s, _):
            to = at_block(s, half)
            for ref, side in ((keep_ref, core), (give_ref, 1 - core)):
                r = at_block(2 * s + side, half)
                ref[to, :SLOT] = dk_ref[r, :] * scale
                ref[to, SLOT:] = dv_ref[r, :]
            return 0

        lax.fori_loop(0, dk_ref.shape[0] // shard, finish, 0)


def attention(place, x, far, near, w_dkv, wq, wr, gain, uk, uv, g, scale, shard, nope, rope, n):
    seq, d_model = x.shape
    rank, vd = w_dkv.shape[1], g.shape[1]
    half, nq, bk = shard // 2, seq // 2, seq // n
    bq = nq // n
    vmem = lambda *shape: pltpu.VMEM(shape, F32)
    packed = lambda *shape: pltpu.VMEM(shape, BF16)
    return pl.pallas_call(
        functools.partial(attn_kernel, scale, shard, half, nope, rope),
        grid_spec=pltpu.PrefetchScalarGridSpec(
            num_scalar_prefetch=1, grid=(n,),
            in_specs=[rows(bk, d_model), whole(*far.shape), whole(*near.shape), whole(*w_dkv.shape), pl.BlockSpec((1, *wq.shape[1:]), lambda i, c: (c[1], 0, 0)),
                      whole(*wr.shape), whole(*gain.shape), whole(*uk.shape), whole(*uv.shape), rows(bq, vd)],
            out_specs=[rows(bq, vd + SLOT), whole(nq, SLOT + vd), whole(nq, SLOT + vd), rows(bk, rank)],
            scratch_shapes=[packed(d_model, SLOT), packed(rank, nope + vd), packed(bq, SLOT), packed(seq, SLOT), packed(seq, vd),
                            vmem(bq, LANES), vmem(bq, LANES), vmem(bq, seq), vmem(bq, LANES), vmem(bq, LANES), packed(bq, vd), vmem(bq, LANES), vmem(bq, SLOT),
                            vmem(seq, SLOT), vmem(seq, vd)]),
        out_shape=[struct((nq, vd + SLOT), BF16), struct((nq, SLOT + vd)), struct((nq, SLOT + vd)), struct((seq, rank), BF16)],
        compiler_params=compiler_params(),
        cost_estimate=cost(2 * seq * d_model * (rank + SLOT) + 7 * nq * seq * SLOT, 2 * x.size, nq * seq),
    )(place, x, far, near, w_dkv, wq, wr, gain, uk, uv, g)


def ring_kernel(side, counts, make, n_given, n_made, *refs):
    n_ring, n_each, n_same = counts
    total = sum(counts)
    given = refs[:n_given]
    srcs, outs = refs[n_given:n_given + total - n_made], refs[n_given + total - n_made:n_given + 2 * total - n_made]
    send_sem, recv_sem, own_sem, *rest = refs[n_given + 2 * total - n_made:]
    direct_sem, made = rest[:2], rest[2:]
    srcs = [*srcs, *made[:n_made]]
    n_dev = 2 * side * side
    me = lax.axis_index("cp")
    pos = ((me // 2) % side, me // (2 * side))
    mesh_id = pl.DeviceIdType.MESH

    def at(dx, dy):
        return (lax.rem(pos[1] + dy + side, side) * side + lax.rem(pos[0] + dx + side, side)) * 2 + me % 2

    def shifted(color, first, second):
        return at(second, first) if color else at(first, second)

    sibling = me + 1 - 2 * (me % 2)
    direct = n_each + n_same > 0
    neighbours = [shifted(color, d, 0) for color in range(2) for d in (1, -1)]
    barrier = pltpu.get_barrier_semaphore()

    def greet(peer):
        pl.semaphore_signal(barrier, inc=1, device_id={"cp": peer}, device_id_type=mesh_id)

    def others(do):
        def body(d, _):
            do(d)
            return 0

        lax.fori_loop(1, n_dev, body, 0)

    if direct:
        others(lambda d: greet(me ^ d))
        pl.semaphore_wait(barrier, n_dev - 1)
    else:
        for peer in (*neighbours, sibling):
            greet(peer)
        pl.semaphore_wait(barrier, len(neighbours) + 1)

    def part(ref, color, piece=0, pieces=1):
        size = ref.shape[0] // (2 * pieces)
        return ref.at[pl.ds((pieces * color + piece) * size, size)]

    def copy(src, dst, sems, peer):
        return pltpu.make_async_remote_copy(src_ref=src, dst_ref=dst, send_sem=sems[0], recv_sem=sems[1], device_id={"cp": peer}, device_id_type=mesh_id)

    def sems(k, color, event):
        return send_sem.at[k, color, event], recv_sem.at[k, color, event]

    pending = []

    def send(color, event, block, peer, *piece):
        for k in range(n_ring):
            src, dst = (srcs[k], outs[k].at[me]) if block is None else (outs[k].at[block],) * 2
            pending.append(copy(part(src, color, *piece), part(dst, color, *piece), sems(k, color, event), peer))
            pending[-1].start()

    def arrived(color, event, block, *piece):
        for k in range(n_ring):
            ref = part(outs[k].at[block], color, *piece)
            copy(ref, ref, sems(k, color, event), sibling).wait_recv()

    own = [pltpu.make_async_copy(srcs[k].at[me] if n_ring <= k < n_ring + n_each else srcs[k], outs[k].at[me], own_sem.at[k]) for k in range(total)]

    def straight(d):
        for k in range(n_ring, total):
            src = srcs[k].at[me ^ d] if k < n_ring + n_each else srcs[k]
            yield copy(src, outs[k].at[me], [s.at[k - n_ring, d] for s in direct_sem], me ^ d)

    def start_direct():
        for c in own[n_ring:]:
            c.start()
        if direct:
            others(lambda d: [c.start() for c in straight(d)])

    def wait_all():
        for c in own:
            c.wait()
        if direct:
            others(lambda d: [c.wait() for c in straight(d)])

    for c in own[:n_ring]:
        c.start()
    if not make:
        start_direct()
    finish = make(*given, *made) if make else None

    colors = range(2)
    offsets = (0, -1, 1, 2)
    first_out, relays, second_out, to_sibling, column = 0, 2, 4, 20, 24

    def spread(c, j, block):
        for d, way in enumerate((1, -1)):
            send(c, second_out + 4 * j + d, block, shifted(c, 0, way))
        send(c, to_sibling + j, block, sibling)

    def relay(c, j):
        for d, way in enumerate((1, -1)):
            block = shifted(c, offsets[j], -way)
            arrived(c, second_out + 4 * j + d, block)
            send(c, second_out + relays + 4 * j + d, block, shifted(c, 0, way), d, 2)
            send(c, column + 3 * j + d, block, sibling)

    if not n_ring:
        wait_all()
        return
    for c in colors:
        for d, way in enumerate((1, -1)):
            send(c, first_out + d, None, shifted(c, way, 0))
        spread(c, 0, None)
    for c in colors:
        for d, way in enumerate((1, -1)):
            block = shifted(c, -way, 0)
            arrived(c, first_out + d, block)
            send(c, relays + d, block, shifted(c, way, 0), d, 2)
            spread(c, 1 + d, block)
    for c in colors:
        relay(c, 0)
    if make:
        finish()
    for c in colors:
        across = shifted(c, 2, 0)
        for d in range(2):
            arrived(c, relays + d, across, d, 2)
        spread(c, 3, across)
    if make:
        start_direct()
    for j in range(1, 4):
        for c in colors:
            relay(c, j)
    for j in range(4):
        for c in colors:
            across = shifted(c, offsets[j], 2)
            for d in range(2):
                arrived(c, second_out + relays + 4 * j + d, across, d, 2)
            send(c, column + 2 + 3 * j, across, sibling)
    other = sibling - me
    for c in colors:
        for j in range(4):
            arrived(c, to_sibling + j, shifted(c, offsets[j], 0) + other)
            for d in range(3):
                arrived(c, column + 3 * j + d, shifted(c, offsets[j], offsets[1 + d]) + other)
    for c in pending:
        c.wait_send()
    wait_all()


def ring_gather(n_dev, cid, ring, each=(), same=(), make=None, given=(), scratch=()):
    side = round((n_dev // 2) ** 0.5)
    sent = [*ring, *each, *same]
    n_made = 1 if make else 0
    shapes = [struct(a.shape if len(ring) <= k < len(ring) + len(each) else (n_dev,) + a.shape, a.dtype) for k, a in enumerate(sent)]
    shapes += [struct(a.shape, a.dtype) for a in scratch[:n_made]]
    counts = len(ring), len(each) + n_made, len(same)
    n_direct = sum(counts[1:])
    dma = pltpu.SemaphoreType.DMA
    in_vmem, anywhere = pl.BlockSpec(memory_space=pltpu.VMEM), pl.BlockSpec(memory_space=pl.ANY)
    return pl.pallas_call(
        functools.partial(ring_kernel, side, counts, make, len(given), n_made),
        in_specs=[anywhere] * len(given) + [in_vmem] * len(sent), out_specs=[anywhere] * len(shapes), out_shape=shapes,
        scratch_shapes=[dma((max(len(ring), 1), 2, EVENTS))] * 2 + [dma((len(shapes),))] + [dma((max(n_direct, 1), n_dev))] * 2 + list(scratch),
        compiler_params=compiler_params(collective_id=cid, has_side_effects=True),
        cost_estimate=cost(4e10),
    )(*given, *sent)


def make_d_out(gy_ref, w_ref, blocks_ref, gy_vmem, w_vmem, sems):
    reads = [pltpu.make_async_copy(src, dst, sems.at[k]) for k, (src, dst) in enumerate(((gy_ref, gy_vmem), (w_ref, w_vmem)))]
    for c in reads:
        c.start()

    def compute():
        for c in reads:
            c.wait()
        heads, v_dim = w_ref.shape[:2]
        half = blocks_ref.shape[1]

        def two_heads(b, _):
            w = w_vmem[pl.ds(2 * b, 2)].reshape(2 * v_dim, -1)
            g = over_cols(gy_vmem[...], w).astype(BF16)
            for h in range(2):
                for core in range(2):
                    blocks_ref[4 * b + 2 * h + core] = g[core * half:(core + 1) * half, h * v_dim:(h + 1) * v_dim]
            return 0

        lax.fori_loop(0, heads // 2, two_heads, 0)

    return compute


def query_grads_kernel(qk_dim, core_ref, x_ref, odq_ref, keep_ref, give_ref, q_acc):
    i = pl.program_id(0)
    core = core_ref[0]
    d_model = x_ref.shape[-1]

    @pl.when(i == 0)
    def _():
        zero(q_acc)

    x = x_ref[...].reshape(-1, d_model)
    dq_t = odq_ref[...].T[-SLOT:][:qk_dim]
    for c in range(4):
        cols = slice(c * d_model // 4, (c + 1) * d_model // 4)
        q_acc[:, cols] += exact(dq_t, x[:, cols])

    @pl.when(i == pl.num_programs(0) - 1)
    def _():
        for ref, side in ((keep_ref, core), (give_ref, 1 - core)):
            ref[...] = q_acc[at_block(side, qk_dim // 2), :]


def output_grads_kernel(core_ref, gy_ref, odq_ref, keep_ref, give_ref, o_acc):
    i = pl.program_id(0)
    core = core_ref[0]
    vd, d_model = o_acc.shape

    @pl.when(i == 0)
    def _():
        zero(o_acc)

    gy = gy_ref[...].reshape(-1, d_model)
    o_t = odq_ref[...].T[:vd]
    for c in range(4):
        cols = slice(c * d_model // 4, (c + 1) * d_model // 4)
        o_acc[:, cols] += exact(o_t, gy[:, cols])

    @pl.when(i == pl.num_programs(0) - 1)
    def _():
        for ref, side in ((keep_ref, core), (give_ref, 1 - core)):
            ref[...] = o_acc[at_block(side, vd // 2), :]


def head_grads(kernel, core, act, odq, n_dev, half, width):
    n = 4
    shards = n_dev // n
    d_model = act.shape[1]
    out = width // 2, d_model
    return pl.pallas_call(
        kernel,
        grid_spec=pltpu.PrefetchScalarGridSpec(
            num_scalar_prefetch=1, grid=(n,),
            in_specs=[pl.BlockSpec((shards, 1, half, d_model), lambda i, c: (i, c[0], 0, 0)), rows(shards * half, odq.shape[1])],
            out_specs=[whole(*out)] * 2, scratch_shapes=[pltpu.VMEM((width, d_model), F32)]),
        out_shape=[struct(out)] * 2, compiler_params=compiler_params(), cost_estimate=cost(act.size * width, act.size),
    )(core[None], act.reshape(n_dev, 2, half, d_model), odq)


def up_grads_kernel(core_ref, latent_ref, kv_ref, keep_ref, give_ref):
    core = core_ref[0]
    up = over_rows(latent_ref[...].reshape(-1, latent_ref.shape[-1]), kv_ref[...])
    count = keep_ref.shape[0]
    width = up.shape[1]
    blocks = keep_ref.shape[1] // width
    for a in range(blocks):
        lo, hi = (up[(s * blocks + a) * count:(s * blocks + a + 1) * count] for s in range(2))
        cols = slice(a * width, (a + 1) * width)
        keep_ref[:, cols] = jnp.where(core == 0, lo, hi)
        give_ref[:, cols] = jnp.where(core == 0, hi, lo)


def up_grads(core, latent, kv, d_model, n_dev, half):
    rank, width = latent.shape[1], kv.shape[1]
    out = rank * width // (2 * d_model), d_model
    return pl.pallas_call(
        up_grads_kernel,
        grid_spec=pltpu.PrefetchScalarGridSpec(
            num_scalar_prefetch=1, grid=(1,),
            in_specs=[pl.BlockSpec((n_dev, 1, half, rank), lambda i, c: (0, c[0], 0, 0)), whole(*kv.shape)], out_specs=[whole(*out)] * 2),
        out_shape=[struct(out)] * 2, compiler_params=compiler_params(), cost_estimate=cost(2 * kv.size * rank, latent.size),
    )(core[None], latent.reshape(n_dev, 2, half, rank), kv)


def low_grads_kernel(x_ref, low_ref, dkv_ref, kr_ref, low_t):
    @pl.when(pl.program_id(0) == 0)
    def _():
        n_dev, _, shard = low_ref.shape
        for d in range(n_dev):
            low_t[:, d * shard:(d + 1) * shard] = low_ref[d]

    g = exact(low_t[...], x_ref[...])
    rank = dkv_ref.shape[1]
    dkv_ref[...] = g[:rank].T
    kr_ref[...] = g[rank:]


def low_grads(x, low, rank):
    seq, d_model = x.shape
    width = low.shape[1]
    rope = width - rank
    cols = 2 * SLOT
    return pl.pallas_call(
        low_grads_kernel, grid=(d_model // cols,),
        in_specs=[pl.BlockSpec((seq, cols), lambda i: (0, i)), whole(*low.shape)],
        out_specs=[rows(cols, rank), pl.BlockSpec((rope, cols), lambda i: (0, i))],
        out_shape=[struct((d_model, rank)), struct((rope, d_model))],
        scratch_shapes=[pltpu.VMEM((width, seq), BF16)],
        compiler_params=compiler_params(), cost_estimate=cost(2 * x.size * width, 2 * x.size),
    )(x, low)


def copy_kernel(src_ref, dst_ref):
    dst_ref[...] = src_ref[...]


def copied(a):
    steps = 4
    block = rows(a.shape[0] // steps, a.shape[1])
    return pl.pallas_call(copy_kernel, grid=(steps,), in_specs=[block], out_specs=block, out_shape=struct(a.shape, a.dtype),
                          compiler_params=compiler_params(), cost_estimate=cost(1e9, 8 * a.size))(a)


def spread_heads_kernel(up_ref, uk_ref, uv_ref):
    heads, _, count, cols = up_ref.shape
    for a, block in enumerate(jnp.split(up_ref[...].reshape(heads, count, cols), cols // SLOT, axis=2)):
        for ref, value in zip((uk_ref, uv_ref), jnp.split(block, 2, axis=2)):
            ref[a * count:(a + 1) * count] = jnp.swapaxes(value, 0, 1)


def spread_heads(up, rank, width):
    heads, _, count, cols = up.shape
    steps = 2
    return pl.pallas_call(
        spread_heads_kernel, grid=(2, steps),
        in_specs=[pl.BlockSpec((heads, 1, count, cols // steps), lambda s, a: (0, s, 0, a))],
        out_specs=[pl.BlockSpec((rank // (2 * steps), heads, width), lambda s, a: (s * steps + a, 0, 0))] * 2,
        out_shape=[struct((rank, heads, width))] * 2, compiler_params=compiler_params(), cost_estimate=cost(1e9, 8 * up.size),
    )(up)


def solution(mesh):
    n_dev = mesh.shape['cp']
    row_spec, per_group = P(('dp', 'cp')), P('dp')
    siblings = [(i, i ^ 1) for i in range(n_dev)]

    def block(x_loc, gy_loc, w_q, w_dkv, g_kv, w_kr, w_uk, w_uv, w_o):
        shard, d_model = x_loc.shape
        heads, qk_dim = w_q.shape[1:]
        rank, _, nope = w_uk.shape
        v_dim, rope = w_uv.shape[2], w_kr.shape[1]
        half, seq = shard // 2, n_dev * shard
        me = lax.axis_index('cp')
        head, core = me // 2, me % 2

        def gather(a):
            return lax.all_gather(a, 'cp', axis=0, tiled=True)

        def summed(keep, give):
            return keep + lax.ppermute(give, 'cp', siblings)

        packed = lambda *shape: pltpu.VMEM(shape, BF16)
        scratch = packed(n_dev, half, v_dim), packed(*gy_loc.shape), packed(*w_o.shape), pltpu.SemaphoreType.DMA((2,))
        x_all, d_out = ring_gather(n_dev, 1, [x_loc], make=make_d_out, given=[gy_loc, w_o], scratch=scratch)
        x_all, d_out = x_all.reshape(seq, d_model), d_out.reshape(seq // 2, v_dim)
        gy_all = gather(lax.optimization_barrier((gy_loc, x_all))[0])

        pick = lambda a, axis: lax.dynamic_index_in_dim(a, head, axis, False)
        uk, uv = pick(w_uk, 1), pick(w_uv, 1)
        w_uk, w_uv, _ = lax.optimization_barrier((w_uk, w_uv, x_all))

        def table(positions):
            return np.concatenate([t for t in rope_tables(positions.astype(np.float32), rope, np) for _ in range(LANES // rope)], axis=1)

        far, near = table(np.arange(0, seq, 4 * shard)), table(np.arange(4 * shard))
        gain = g_kv.astype(F32)[None]
        odq, kv_keep, kv_give, latent = attention(jnp.stack([core, head]), x_all, far, near, w_dkv, w_q.transpose(1, 2, 0), w_kr.T, gain, uk, uv, d_out, qk_dim ** -0.5, shard, nope, rope, 4)

        def exchange(a):
            return lax.all_to_all(a.reshape(n_dev, half, -1), 'cp', 0, 0, tiled=True).reshape(heads, shard, -1)

        got_odq = exchange(odq)
        q_keep, q_give = head_grads(functools.partial(query_grads_kernel, qk_dim), core, x_all, odq, n_dev, half, qk_dim)
        q_my = summed(q_keep, q_give)
        gwq = gather(q_my)

        kv_sum = lax.optimization_barrier((summed(kv_keep, kv_give), q_keep))[0]
        kv_my = jnp.concatenate([kv_sum[:, :nope], kv_sum[:, SLOT:]], axis=1).astype(BF16)
        dkr_my = kv_sum[:, nope:qk_dim].reshape(n_dev, half * rope // LANES, LANES)
        o_keep, o_give = head_grads(output_grads_kernel, core, gy_all, odq, n_dev, half, v_dim)
        o_my = summed(o_keep, o_give)
        gwo = gather(o_my)
        got_odq, kv_my, _ = lax.optimization_barrier((got_odq, kv_my, o_keep))
        got_kv = exchange(kv_my)
        up_keep, up_give = up_grads(core, latent, kv_my, d_model, n_dev, half)
        up_my = summed(up_keep, up_give)
        o_loc, dq_loc, _ = jnp.split(got_odq, [v_dim, v_dim + qk_dim], axis=2)
        y_loc = jnp.einsum('htv,hvd->td', o_loc, w_o, preferred_element_type=F32).astype(BF16)
        dx_loc = jnp.einsum('hte,dhe->td', dq_loc, w_q, preferred_element_type=F32)
        dkr_my, y_loc, dx_loc, _, _ = lax.optimization_barrier((dkr_my, y_loc, dx_loc, o_my, up_my))
        got_r, = ring_gather(n_dev, 2, [], [dkr_my])
        got_kv, got_r = lax.optimization_barrier((got_kv, got_r))
        dkr_loc = jnp.sum(got_r.reshape(heads, shard, rope), axis=0)
        dk_loc, dv_loc = jnp.split(got_kv, [nope], axis=2)
        d_latent = jnp.einsum('htn,chn->tc', dk_loc, w_uk, preferred_element_type=F32) + jnp.einsum('htv,chv->tc', dv_loc, w_uv, preferred_element_type=F32)
        c_loc = exact(x_loc, w_dkv)
        inv_loc = lax.rsqrt(jnp.mean(c_loc * c_loc, axis=-1, keepdims=True) + NORM_EPS)
        c_norm = c_loc * inv_loc
        gg_part = jnp.sum(d_latent * c_norm, axis=0)
        d_norm = d_latent * gain
        dc_loc = (inv_loc * (d_norm - c_norm * jnp.mean(d_norm * c_norm, axis=-1, keepdims=True))).astype(BF16)
        cos_t, sin_t = rope_tables((me * shard + jnp.arange(shard)).astype(F32), rope)
        dkr_raw = rope_back(dkr_loc, cos_t, sin_t).astype(BF16)
        dx_loc = dx_loc + jnp.einsum('tc,dc->td', dc_loc, w_dkv, preferred_element_type=F32) + jnp.einsum('tr,dr->td', dkr_raw, w_kr, preferred_element_type=F32)

        gg_rows = rank // LANES
        gg_part = jnp.pad(gg_part.reshape(gg_rows, LANES), ((0, 8 - gg_rows), (0, 0)))
        low, up, gg = ring_gather(n_dev, 3, [jnp.concatenate([dc_loc, dkr_raw], axis=1).T, up_my], (), [gg_part])
        gw_dkv, gw_kr = low_grads(x_all, low, rank)
        gg_kv = jnp.sum(gg, axis=0)[:gg_rows].reshape(rank)
        gwq = copied(gwq)
        gw_uk, gw_uv = spread_heads(up.reshape(heads, 2, -1, d_model), rank, nope)
        gw_q = gwq.reshape(heads, qk_dim, d_model).transpose(2, 0, 1)
        return y_loc, dx_loc.astype(BF16), gw_q, gw_dkv, gg_kv, gw_kr.T, gw_uk, gw_uv, gwo.reshape(heads, v_dim, d_model)

    return jax.shard_map(block, mesh=mesh, in_specs=(row_spec, row_spec) + (P(),) * 7, out_specs=(row_spec, row_spec) + (per_group,) * 7, check_vma=False)
```

```python
import functools

import jax
import jax.numpy as jnp
import numpy as np
from jax import lax
from jax.experimental import pallas as pl
from jax.experimental.pallas import tpu as pltpu
from jax.sharding import PartitionSpec as P


ROPE_THETA = 10000.0
NORM_EPS = 1e-6
LOG2E = 1.4426950408889634
MASKED = -1e30
F32 = jnp.float32
BF16 = jnp.bfloat16
OVER_ROWS = (((0,), (0,)), ((), ()))
OVER_COLS = (((1,), (1,)), ((), ()))
LANES = 128
SLOT = 2 * LANES
VMEM_LIMIT = 63 * 1024 * 1024
EVENTS = 36


def compiler_params(**more):
    return pltpu.CompilerParams(vmem_limit_bytes=VMEM_LIMIT, **more)


def cost(flops, bytes_accessed=0, transcendentals=0):
    return pl.CostEstimate(flops=int(flops), bytes_accessed=bytes_accessed, transcendentals=transcendentals)


def struct(shape, dtype=F32):
    return jax.ShapeDtypeStruct(shape, dtype)


def whole(*shape):
    return pl.BlockSpec(shape, lambda *i: (0,) * len(shape))


def rows(count, width):
    return pl.BlockSpec((count, width), lambda i, *_: (i, 0))


def zero(*refs):
    for ref in refs:
        ref[...] = jnp.zeros(ref.shape, ref.dtype)


def exact(a, b):
    return jnp.dot(a, b, preferred_element_type=F32)


def over_rows(a, b):
    return lax.dot_general(a, b, OVER_ROWS, preferred_element_type=F32)


def over_cols(a, b):
    return lax.dot_general(a, b, OVER_COLS, preferred_element_type=F32)


def at_block(index, size):
    return pl.ds(pl.multiple_of(index * size, size), size)


def rope_tables(positions, rope_dim, xp=jnp):
    half_dim = rope_dim // 2
    inv_freq = ROPE_THETA ** (-(xp.arange(half_dim, dtype=xp.float32) * 2.0 / rope_dim))
    angles = positions[:, None] * inv_freq[None, :]
    return xp.cos(angles), xp.sin(angles)


def rope_back(g_in, cos_t, sin_t):
    first_half, second_half = jnp.split(g_in, 2, axis=-1)
    return jnp.concatenate([first_half * cos_t + second_half * sin_t, second_half * cos_t - first_half * sin_t], axis=-1)


def attn_kernel(scale, shard, half, nope, rope, place_ref, x_ref, far_ref, near_ref, w_ref, wq_ref, wr_ref, gain_ref, uk_ref, uv_ref, g_ref,
                odq_ref, sent_ref, keep_ref, give_ref, latent_ref,
                w2_ref, wkv_ref, q_ref, k_ref, v_ref, cm_ref, sm_ref, s_ref, m_ref, l_ref, do_ref, d_ref, acc_ref, dk_ref, dv_ref):
    i = pl.program_id(0)
    n = pl.num_programs(0)
    core = place_ref[0]
    bq = q_ref.shape[0]
    bk = x_ref.shape[0]
    vd = v_ref.shape[1]
    rep = bk // LANES

    def keys(j):
        return at_block(j, bk)

    def wide(x):
        return jnp.concatenate([x] * rep, axis=1)

    def fold(x, op):
        return functools.reduce(op, jnp.split(x, rep, axis=1))

    def swapped(t):
        lane = lax.broadcasted_iota(jnp.int32, t.shape, 1)
        return jnp.where(lane % rope < rope // 2, pltpu.roll(t, LANES - rope // 2, 1), pltpu.roll(t, rope // 2, 1))

    def both_tables(t):
        first = lax.broadcasted_iota(jnp.int32, t.shape, 1) < rope
        other = pltpu.roll(t, rope, 1)
        return jnp.where(first, t, other), jnp.where(first, other, t)

    def spread(ref, column):
        ref[...] = jnp.broadcast_to(column, ref.shape)

    @pl.when(i == 0)
    def _():
        w2_ref[...] = jnp.concatenate([wq_ref[0], wr_ref[...]], axis=0).T
        wkv_ref[:, :nope] = uk_ref[...]
        wkv_ref[:, nope:] = uv_ref[...]
        zero(dk_ref, dv_ref)

    step = near_ref.shape[0]

    def project(b, _):
        r = at_block(b, step)
        t = at_block(i * (bk // step) + b, step)
        x = x_ref[r, :]
        c = exact(x, w_ref[...])
        inv = lax.rsqrt(jnp.sum(c * c, axis=1, keepdims=True) * (1.0 / c.shape[1]) + NORM_EPS)
        latent = (c * inv * gain_ref[...]).astype(BF16)
        latent_ref[r, :] = latent
        kv = exact(latent, wkv_ref[...])
        v_ref[t, :] = kv[:, nope:].astype(BF16)
        qk = exact(x, w2_ref[...])
        far = far_ref[pl.ds(i * (bk // step) + b, 1), :]
        lane = lax.broadcasted_iota(jnp.int32, (step, LANES), 1)
        (cos_a, sin_a), (cos_b, sin_b) = both_tables(far), both_tables(near_ref[...])
        cos_t = cos_a * cos_b - sin_a * sin_b
        sin_t = sin_a * cos_b + cos_a * sin_b
        sin_t = jnp.where(lane % rope < rope // 2, -sin_t, sin_t)
        turned = qk[:, nope:]
        turned = turned * cos_t + swapped(turned) * sin_t
        k_ref[t, :] = jnp.concatenate([kv[:, :nope], jnp.where(lane < rope, pltpu.roll(turned, rope, 1), 0.0)], axis=1).astype(BF16)
        q = jnp.concatenate([qk[:, :nope], jnp.where(lane < rope, turned, 0.0)], axis=1).astype(BF16)
        for a in range(step // shard):
            to = at_block(b * (step // shard) + a, half)
            lo, hi = slice(a * shard, a * shard + half), slice(a * shard + half, (a + 1) * shard)
            for ref, value in ((q_ref, q), (cm_ref, cos_t), (sm_ref, sin_t)):
                ref[to, :] = jnp.where(core == 0, value[lo], value[hi])
        return 0

    lax.fori_loop(0, bk // step, project, 0)

    m_ref[...] = jnp.full(m_ref.shape, MASKED, F32)

    def scores(j):
        return over_cols(q_ref[...], k_ref[keys(j), :])

    def note(j, s):
        s_ref[:, keys(j)] = s
        m_ref[...] = jnp.maximum(m_ref[...], fold(s, jnp.maximum))

    def full_tile(j, _):
        note(j, scores(j))
        return 0

    lax.fori_loop(0, i, full_tile, 0)
    row = lax.broadcasted_iota(jnp.int32, (bq, bk), 0)
    col = lax.broadcasted_iota(jnp.int32, (bq, bk), 1)
    note(i, jnp.where(col <= (row // half) * shard + core * half + row % half, scores(i), MASKED))

    spread(m_ref, jnp.max(m_ref[...], axis=1, keepdims=True))
    zero(l_ref, acc_ref)

    def prob_tile(j, _):
        r = keys(j)
        p = jnp.exp2((s_ref[:, r] - wide(m_ref[...])) * (scale * LOG2E))
        s_ref[:, r] = p
        l_ref[...] += fold(p, jnp.add)
        acc_ref[:, :vd] += exact(p.astype(BF16), v_ref[r, :])
        return 0

    lax.fori_loop(0, i + 1, prob_tile, 0)

    inv = 1.0 / jnp.sum(l_ref[...], axis=1, keepdims=True)
    o = acc_ref[:, :vd] * inv
    odq_ref[:, :vd] = o.astype(BF16)
    do = g_ref[...].astype(F32)
    spread(d_ref, jnp.sum(do * o, axis=1, keepdims=True) * inv)
    do_ref[...] = (do * inv).astype(BF16)
    zero(acc_ref)

    def back_tile(j, _):
        r = keys(j)
        p = s_ref[:, r]
        dp = over_cols(do_ref[...], v_ref[r, :])
        ds = (p * (dp - wide(d_ref[...]))).astype(BF16)
        dv_ref[r, :] += over_rows(p.astype(BF16), do_ref[...])
        dk_ref[r, :] += over_rows(ds, q_ref[...])
        acc_ref[...] += exact(ds, k_ref[r, :])
        return 0

    lax.fori_loop(0, i + 1, back_tile, 0)
    dq = acc_ref[...] * scale
    turned = dq[:, nope:]
    turned = turned * cm_ref[...] - swapped(turned) * sm_ref[...]
    odq_ref[:, vd:vd + nope] = dq[:, :nope].astype(BF16)
    odq_ref[:, vd + nope:] = turned.astype(BF16)
    sent_ref[:, :half] = o.astype(BF16).reshape(-1, half, LANES)
    sent_ref[:, half:2 * half] = dq[:, :nope].astype(BF16).reshape(-1, half, LANES)
    turned = turned.reshape(-1, half, LANES)
    low, high = turned[:, :half // 2], turned[:, half // 2:]
    lane = lax.broadcasted_iota(jnp.int32, low.shape, 2)
    sent_ref[:, 2 * half:] = jnp.where(lane < rope, low, pltpu.roll(high, rope, 2)).astype(BF16)

    @pl.when(i == n - 1)
    def _():
        def finish(s, _):
            to = at_block(s, half)
            for ref, side in ((keep_ref, core), (give_ref, 1 - core)):
                r = at_block(2 * s + side, half)
                ref[to, :SLOT] = dk_ref[r, :] * scale
                ref[to, SLOT:] = dv_ref[r, :]
            return 0

        lax.fori_loop(0, dk_ref.shape[0] // shard, finish, 0)


def attention(place, x, far, near, w_dkv, wq, wr, gain, uk, uv, g, scale, shard, nope, rope, n):
    seq, d_model = x.shape
    rank, vd = w_dkv.shape[1], g.shape[1]
    half, nq, bk = shard // 2, seq // 2, seq // n
    bq = nq // n
    sent = seq // shard, 2 * half + half // 2, LANES
    vmem = lambda *shape: pltpu.VMEM(shape, F32)
    packed = lambda *shape: pltpu.VMEM(shape, BF16)
    return pl.pallas_call(
        functools.partial(attn_kernel, scale, shard, half, nope, rope),
        grid_spec=pltpu.PrefetchScalarGridSpec(
            num_scalar_prefetch=1, grid=(n,),
            in_specs=[rows(bk, d_model), whole(*far.shape), whole(*near.shape), whole(*w_dkv.shape), pl.BlockSpec((1, *wq.shape[1:]), lambda i, c: (c[1], 0, 0)),
                      whole(*wr.shape), whole(*gain.shape), whole(*uk.shape), whole(*uv.shape), rows(bq, vd)],
            out_specs=[rows(bq, vd + SLOT), pl.BlockSpec((sent[0] // n, *sent[1:]), lambda i, c: (i, 0, 0)), whole(nq, SLOT + vd), whole(nq, SLOT + vd), rows(bk, rank)],
            scratch_shapes=[packed(d_model, SLOT), packed(rank, nope + vd), packed(bq, SLOT), packed(seq, SLOT), packed(seq, vd),
                            vmem(bq, LANES), vmem(bq, LANES), vmem(bq, seq), vmem(bq, LANES), vmem(bq, LANES), packed(bq, vd), vmem(bq, LANES), vmem(bq, SLOT),
                            vmem(seq, SLOT), vmem(seq, vd)]),
        out_shape=[struct((nq, vd + SLOT), BF16), struct(sent, BF16), struct((nq, SLOT + vd)), struct((nq, SLOT + vd)), struct((seq, rank), BF16)],
        compiler_params=compiler_params(),
        cost_estimate=cost(2 * seq * d_model * (rank + SLOT) + 7 * nq * seq * SLOT, 2 * x.size, nq * seq),
    )(place, x, far, near, w_dkv, wq, wr, gain, uk, uv, g)


def ring_kernel(side, counts, make, n_given, n_made, *refs):
    n_ring, n_each, n_same = counts
    total = sum(counts)
    given = refs[:n_given]
    srcs, outs = refs[n_given:n_given + total - n_made], refs[n_given + total - n_made:n_given + 2 * total - n_made]
    send_sem, recv_sem, own_sem, *rest = refs[n_given + 2 * total - n_made:]
    direct_sem, made = rest[:2], rest[2:]
    srcs = [*srcs, *made[:n_made]]
    n_dev = 2 * side * side
    me = lax.axis_index("cp")
    pos = ((me // 2) % side, me // (2 * side))
    mesh_id = pl.DeviceIdType.MESH

    def at(dx, dy):
        return (lax.rem(pos[1] + dy + side, side) * side + lax.rem(pos[0] + dx + side, side)) * 2 + me % 2

    def shifted(color, first, second):
        return at(second, first) if color else at(first, second)

    sibling = me + 1 - 2 * (me % 2)
    direct = n_each + n_same > 0
    neighbours = [shifted(color, d, 0) for color in range(2) for d in (1, -1)]
    barrier = pltpu.get_barrier_semaphore()

    def greet(peer):
        pl.semaphore_signal(barrier, inc=1, device_id={"cp": peer}, device_id_type=mesh_id)

    def others(do):
        def body(d, _):
            do(d)
            return 0

        lax.fori_loop(1, n_dev, body, 0)

    if direct:
        others(lambda d: greet(me ^ d))
        pl.semaphore_wait(barrier, n_dev - 1)
    else:
        for peer in (*neighbours, sibling):
            greet(peer)
        pl.semaphore_wait(barrier, len(neighbours) + 1)

    def part(ref, color, piece=0, pieces=1):
        size = ref.shape[0] // (2 * pieces)
        return ref.at[pl.ds((pieces * color + piece) * size, size)]

    def copy(src, dst, sems, peer):
        return pltpu.make_async_remote_copy(src_ref=src, dst_ref=dst, send_sem=sems[0], recv_sem=sems[1], device_id={"cp": peer}, device_id_type=mesh_id)

    def sems(k, color, event):
        return send_sem.at[k, color, event], recv_sem.at[k, color, event]

    pending = []

    def send(color, event, block, peer, *piece):
        for k in range(n_ring):
            src, dst = (srcs[k], outs[k].at[me]) if block is None else (outs[k].at[block],) * 2
            pending.append(copy(part(src, color, *piece), part(dst, color, *piece), sems(k, color, event), peer))
            pending[-1].start()

    def arrived(color, event, block, *piece):
        for k in range(n_ring):
            ref = part(outs[k].at[block], color, *piece)
            copy(ref, ref, sems(k, color, event), sibling).wait_recv()

    own = [pltpu.make_async_copy(srcs[k].at[me] if n_ring <= k < n_ring + n_each else srcs[k], outs[k].at[me], own_sem.at[k]) for k in range(total)]

    def straight(d):
        for k in range(n_ring, total):
            src = srcs[k].at[me ^ d] if k < n_ring + n_each else srcs[k]
            yield copy(src, outs[k].at[me], [s.at[k - n_ring, d] for s in direct_sem], me ^ d)

    def start_direct():
        for c in own[n_ring:]:
            c.start()
        if direct:
            others(lambda d: [c.start() for c in straight(d)])

    def wait_all():
        for c in own:
            c.wait()
        if direct:
            others(lambda d: [c.wait() for c in straight(d)])

    for c in own[:n_ring]:
        c.start()
    if not make:
        start_direct()
    finish = make(*given, *made) if make else None

    colors = range(2)
    offsets = (0, -1, 1, 2)
    first_out, relays, second_out, to_sibling, column = 0, 2, 4, 20, 24

    def spread(c, j, block):
        for d, way in enumerate((1, -1)):
            send(c, second_out + 4 * j + d, block, shifted(c, 0, way))
        send(c, to_sibling + j, block, sibling)

    def relay(c, j):
        for d, way in enumerate((1, -1)):
            block = shifted(c, offsets[j], -way)
            arrived(c, second_out + 4 * j + d, block)
            send(c, second_out + relays + 4 * j + d, block, shifted(c, 0, way), d, 2)
            send(c, column + 3 * j + d, block, sibling)

    if not n_ring:
        wait_all()
        return
    for c in colors:
        for d, way in enumerate((1, -1)):
            send(c, first_out + d, None, shifted(c, way, 0))
        spread(c, 0, None)
    for c in colors:
        for d, way in enumerate((1, -1)):
            block = shifted(c, -way, 0)
            arrived(c, first_out + d, block)
            send(c, relays + d, block, shifted(c, way, 0), d, 2)
            spread(c, 1 + d, block)
    for c in colors:
        relay(c, 0)
    if make:
        finish()
    for c in colors:
        across = shifted(c, 2, 0)
        for d in range(2):
            arrived(c, relays + d, across, d, 2)
        spread(c, 3, across)
    if make:
        start_direct()
    for j in range(1, 4):
        for c in colors:
            relay(c, j)
    for j in range(4):
        for c in colors:
            across = shifted(c, offsets[j], 2)
            for d in range(2):
                arrived(c, second_out + relays + 4 * j + d, across, d, 2)
            send(c, column + 2 + 3 * j, across, sibling)
    other = sibling - me
    for c in colors:
        for j in range(4):
            arrived(c, to_sibling + j, shifted(c, offsets[j], 0) + other)
            for d in range(3):
                arrived(c, column + 3 * j + d, shifted(c, offsets[j], offsets[1 + d]) + other)
    for c in pending:
        c.wait_send()
    wait_all()


def ring_gather(n_dev, cid, ring, each=(), same=(), make=None, given=(), scratch=()):
    side = round((n_dev // 2) ** 0.5)
    sent = [*ring, *each, *same]
    n_made = 1 if make else 0
    shapes = [struct(a.shape if len(ring) <= k < len(ring) + len(each) else (n_dev,) + a.shape, a.dtype) for k, a in enumerate(sent)]
    shapes += [struct(a.shape, a.dtype) for a in scratch[:n_made]]
    counts = len(ring), len(each) + n_made, len(same)
    n_direct = sum(counts[1:])
    dma = pltpu.SemaphoreType.DMA
    in_vmem, anywhere = pl.BlockSpec(memory_space=pltpu.VMEM), pl.BlockSpec(memory_space=pl.ANY)
    return pl.pallas_call(
        functools.partial(ring_kernel, side, counts, make, len(given), n_made),
        in_specs=[anywhere] * len(given) + [in_vmem] * len(sent), out_specs=[anywhere] * len(shapes), out_shape=shapes,
        scratch_shapes=[dma((max(len(ring), 1), 2, EVENTS))] * 2 + [dma((len(shapes),))] + [dma((max(n_direct, 1), n_dev))] * 2 + list(scratch),
        compiler_params=compiler_params(collective_id=cid, has_side_effects=True),
        cost_estimate=cost(4e10),
    )(*given, *sent)


def make_d_out(gy_ref, w_ref, blocks_ref, gy_vmem, w_vmem, sems):
    reads = [pltpu.make_async_copy(src, dst, sems.at[k]) for k, (src, dst) in enumerate(((gy_ref, gy_vmem), (w_ref, w_vmem)))]
    for c in reads:
        c.start()

    def compute():
        for c in reads:
            c.wait()
        heads, v_dim = w_ref.shape[:2]
        half = blocks_ref.shape[1]

        def two_heads(b, _):
            w = w_vmem[pl.ds(2 * b, 2)].reshape(2 * v_dim, -1)
            g = over_cols(gy_vmem[...], w).astype(BF16)
            for h in range(2):
                for core in range(2):
                    blocks_ref[4 * b + 2 * h + core] = g[core * half:(core + 1) * half, h * v_dim:(h + 1) * v_dim]
            return 0

        lax.fori_loop(0, heads // 2, two_heads, 0)

    return compute


def query_grads_kernel(qk_dim, core_ref, x_ref, odq_ref, keep_ref, give_ref, q_acc):
    i = pl.program_id(0)
    core = core_ref[0]
    d_model = x_ref.shape[-1]

    @pl.when(i == 0)
    def _():
        zero(q_acc)

    x = x_ref[...].reshape(-1, d_model)
    dq_t = odq_ref[...].T[-SLOT:][:qk_dim]
    for c in range(4):
        cols = slice(c * d_model // 4, (c + 1) * d_model // 4)
        q_acc[:, cols] += exact(dq_t, x[:, cols])

    @pl.when(i == pl.num_programs(0) - 1)
    def _():
        for ref, side in ((keep_ref, core), (give_ref, 1 - core)):
            ref[...] = q_acc[at_block(side, qk_dim // 2), :]


def output_grads_kernel(core_ref, gy_ref, odq_ref, keep_ref, give_ref, o_acc):
    i = pl.program_id(0)
    core = core_ref[0]
    vd, d_model = o_acc.shape

    @pl.when(i == 0)
    def _():
        zero(o_acc)

    gy = gy_ref[...].reshape(-1, d_model)
    o_t = odq_ref[...].T[:vd]
    for c in range(4):
        cols = slice(c * d_model // 4, (c + 1) * d_model // 4)
        o_acc[:, cols] += exact(o_t, gy[:, cols])

    @pl.when(i == pl.num_programs(0) - 1)
    def _():
        for ref, side in ((keep_ref, core), (give_ref, 1 - core)):
            ref[...] = o_acc[at_block(side, vd // 2), :]


def head_grads(kernel, core, act, odq, n_dev, half, width):
    n = 4
    shards = n_dev // n
    d_model = act.shape[1]
    out = width // 2, d_model
    return pl.pallas_call(
        kernel,
        grid_spec=pltpu.PrefetchScalarGridSpec(
            num_scalar_prefetch=1, grid=(n,),
            in_specs=[pl.BlockSpec((shards, 1, half, d_model), lambda i, c: (i, c[0], 0, 0)), rows(shards * half, odq.shape[1])],
            out_specs=[whole(*out)] * 2, scratch_shapes=[pltpu.VMEM((width, d_model), F32)]),
        out_shape=[struct(out)] * 2, compiler_params=compiler_params(), cost_estimate=cost(act.size * width, act.size),
    )(core[None], act.reshape(n_dev, 2, half, d_model), odq)


def up_grads_kernel(core_ref, latent_ref, kv_ref, keep_ref, give_ref):
    core = core_ref[0]
    up = over_rows(latent_ref[...].reshape(-1, latent_ref.shape[-1]), kv_ref[...])
    count = keep_ref.shape[0]
    width = up.shape[1]
    blocks = keep_ref.shape[1] // width
    for a in range(blocks):
        lo, hi = (up[(s * blocks + a) * count:(s * blocks + a + 1) * count] for s in range(2))
        cols = slice(a * width, (a + 1) * width)
        keep_ref[:, cols] = jnp.where(core == 0, lo, hi)
        give_ref[:, cols] = jnp.where(core == 0, hi, lo)


def up_grads(core, latent, kv, d_model, n_dev, half):
    rank, width = latent.shape[1], kv.shape[1]
    out = rank * width // (2 * d_model), d_model
    return pl.pallas_call(
        up_grads_kernel,
        grid_spec=pltpu.PrefetchScalarGridSpec(
            num_scalar_prefetch=1, grid=(1,),
            in_specs=[pl.BlockSpec((n_dev, 1, half, rank), lambda i, c: (0, c[0], 0, 0)), whole(*kv.shape)], out_specs=[whole(*out)] * 2),
        out_shape=[struct(out)] * 2, compiler_params=compiler_params(), cost_estimate=cost(2 * kv.size * rank, latent.size),
    )(core[None], latent.reshape(n_dev, 2, half, rank), kv)


def finish_kernel(x_ref, low_ref, g_ref, dkv_ref, kr_ref, copy_ref, low_t):
    @pl.when(pl.program_id(0) == 0)
    def _():
        n_dev, _, shard = low_ref.shape
        for d in range(n_dev):
            low_t[:, d * shard:(d + 1) * shard] = low_ref[d]

    g = exact(low_t[...], x_ref[...])
    rank = dkv_ref.shape[1]
    dkv_ref[...] = g[:rank].T
    kr_ref[...] = g[rank:]
    copy_ref[...] = g_ref[...]


def finish(x, low, g, rank):
    seq, d_model = x.shape
    width = low.shape[1]
    rope = width - rank
    steps = 4
    cols = d_model // steps
    piece = rows(g.shape[0] // steps, g.shape[1])
    return pl.pallas_call(
        finish_kernel, grid=(steps,),
        in_specs=[pl.BlockSpec((seq, cols), lambda i: (0, i)), whole(*low.shape), piece],
        out_specs=[rows(cols, rank), pl.BlockSpec((rope, cols), lambda i: (0, i)), piece],
        out_shape=[struct((d_model, rank)), struct((rope, d_model)), struct(g.shape)],
        scratch_shapes=[pltpu.VMEM((width, seq), BF16)],
        compiler_params=compiler_params(), cost_estimate=cost(2 * x.size * width, 2 * x.size + 8 * g.size),
    )(x, low, g)


def spread_heads_kernel(up_ref, uk_ref, uv_ref):
    heads, _, count, cols = up_ref.shape
    for a, block in enumerate(jnp.split(up_ref[...].reshape(heads, count, cols), cols // SLOT, axis=2)):
        for ref, value in zip((uk_ref, uv_ref), jnp.split(block, 2, axis=2)):
            ref[a * count:(a + 1) * count] = jnp.swapaxes(value, 0, 1)


def spread_heads(up, rank, width):
    heads, _, count, cols = up.shape
    steps = 2
    return pl.pallas_call(
        spread_heads_kernel, grid=(2, steps),
        in_specs=[pl.BlockSpec((heads, 1, count, cols // steps), lambda s, a: (0, s, 0, a))],
        out_specs=[pl.BlockSpec((rank // (2 * steps), heads, width), lambda s, a: (s * steps + a, 0, 0))] * 2,
        out_shape=[struct((rank, heads, width))] * 2, compiler_params=compiler_params(), cost_estimate=cost(1e9, 8 * up.size),
    )(up)


def solution(mesh):
    n_dev = mesh.shape['cp']
    row_spec, per_group = P(('dp', 'cp')), P('dp')
    siblings = [(i, i ^ 1) for i in range(n_dev)]

    def block(x_loc, gy_loc, w_q, w_dkv, g_kv, w_kr, w_uk, w_uv, w_o):
        shard, d_model = x_loc.shape
        heads, qk_dim = w_q.shape[1:]
        rank, _, nope = w_uk.shape
        v_dim, rope = w_uv.shape[2], w_kr.shape[1]
        half, seq = shard // 2, n_dev * shard
        me = lax.axis_index('cp')
        head, core = me // 2, me % 2

        def gather(a):
            return lax.all_gather(a, 'cp', axis=0, tiled=True)

        def summed(keep, give):
            return keep + lax.ppermute(give, 'cp', siblings)

        packed = lambda *shape: pltpu.VMEM(shape, BF16)
        scratch = packed(n_dev, half, v_dim), packed(*gy_loc.shape), packed(*w_o.shape), pltpu.SemaphoreType.DMA((2,))
        x_all, d_out = ring_gather(n_dev, 1, [x_loc], make=make_d_out, given=[gy_loc, w_o], scratch=scratch)
        x_all, d_out = x_all.reshape(seq, d_model), d_out.reshape(seq // 2, v_dim)
        gy_all = gather(lax.optimization_barrier((gy_loc, x_all))[0])

        pick = lambda a, axis: lax.dynamic_index_in_dim(a, head, axis, False)
        uk, uv = pick(w_uk, 1), pick(w_uv, 1)
        w_uk, w_uv, _ = lax.optimization_barrier((w_uk, w_uv, x_all))

        def table(positions):
            return np.concatenate([t for t in rope_tables(positions.astype(np.float32), rope, np) for _ in range(LANES // rope)], axis=1)

        far, near = table(np.arange(0, seq, 4 * shard)), table(np.arange(4 * shard))
        gain = g_kv.astype(F32)[None]
        odq, sent, kv_keep, kv_give, latent = attention(jnp.stack([core, head]), x_all, far, near, w_dkv, w_q.transpose(1, 2, 0), w_kr.T, gain, uk, uv, d_out, qk_dim ** -0.5, shard, nope, rope, 4)

        def exchange(a):
            return lax.all_to_all(a, 'cp', 0, 0, tiled=True).reshape(heads, 2, *a.shape[1:])

        got_odq = exchange(sent)
        q_keep, q_give = head_grads(functools.partial(query_grads_kernel, qk_dim), core, x_all, odq, n_dev, half, qk_dim)
        q_my = summed(q_keep, q_give)
        gwq = gather(q_my)

        kv_sum = lax.optimization_barrier((summed(kv_keep, kv_give), q_keep))[0]
        kv_my = jnp.concatenate([kv_sum[:, :nope], kv_sum[:, SLOT:]], axis=1).astype(BF16)
        dkr_my = kv_sum[:, nope:qk_dim].reshape(n_dev, half * rope // LANES, LANES)
        o_keep, o_give = head_grads(output_grads_kernel, core, gy_all, odq, n_dev, half, v_dim)
        o_my = summed(o_keep, o_give)
        gwo = gather(o_my)
        got_odq, kv_my, _ = lax.optimization_barrier((got_odq, kv_my, o_keep))
        got_kv = exchange(kv_my.reshape(n_dev, half, -1))
        up_keep, up_give = up_grads(core, latent, kv_my, d_model, n_dev, half)
        up_my = summed(up_keep, up_give)
        o_loc, dq_loc, dq_rope = jnp.split(got_odq, [half, 2 * half], axis=2)
        dq_loc = jnp.concatenate([dq_loc, jnp.concatenate([dq_rope[..., :rope], dq_rope[..., rope:]], axis=2)], axis=3)
        o_loc, dq_loc = o_loc.reshape(heads, shard, -1), dq_loc.reshape(heads, shard, -1)
        y_loc = jnp.einsum('htv,hvd->td', o_loc, w_o, preferred_element_type=F32).astype(BF16)
        dx_loc = jnp.einsum('hte,dhe->td', dq_loc, w_q, preferred_element_type=F32)
        dkr_my, y_loc, dx_loc, _, _ = lax.optimization_barrier((dkr_my, y_loc, dx_loc, o_my, up_my))
        got_r, = ring_gather(n_dev, 2, [], [dkr_my])
        got_kv, got_r = lax.optimization_barrier((got_kv, got_r))
        dkr_loc = jnp.sum(got_r.reshape(heads, shard, rope), axis=0)
        dk_loc, dv_loc = jnp.split(got_kv.reshape(heads, shard, -1), [nope], axis=2)
        d_latent = jnp.einsum('htn,chn->tc', dk_loc, w_uk, preferred_element_type=F32) + jnp.einsum('htv,chv->tc', dv_loc, w_uv, preferred_element_type=F32)
        c_loc = exact(x_loc, w_dkv)
        inv_loc = lax.rsqrt(jnp.mean(c_loc * c_loc, axis=-1, keepdims=True) + NORM_EPS)
        c_norm = c_loc * inv_loc
        gg_part = jnp.sum(d_latent * c_norm, axis=0)
        d_norm = d_latent * gain
        dc_loc = (inv_loc * (d_norm - c_norm * jnp.mean(d_norm * c_norm, axis=-1, keepdims=True))).astype(BF16)
        cos_t, sin_t = rope_tables((me * shard + jnp.arange(shard)).astype(F32), rope)
        dkr_raw = rope_back(dkr_loc, cos_t, sin_t).astype(BF16)
        dx_loc = dx_loc + jnp.einsum('tc,dc->td', dc_loc, w_dkv, preferred_element_type=F32) + jnp.einsum('tr,dr->td', dkr_raw, w_kr, preferred_element_type=F32)

        gg_rows = rank // LANES
        gg_part = jnp.pad(gg_part.reshape(gg_rows, LANES), ((0, 8 - gg_rows), (0, 0)))
        low_my = jnp.concatenate([dc_loc, dkr_raw], axis=1).T
        low_my, dx_loc = lax.optimization_barrier((low_my, dx_loc.astype(BF16)))
        low, up, gg = ring_gather(n_dev, 3, [low_my, up_my], (), [gg_part])
        gw_dkv, gw_kr, gwq = finish(x_all, low, gwq, rank)
        gg_kv = jnp.sum(gg, axis=0)[:gg_rows].reshape(rank)
        gw_uk, gw_uv = spread_heads(up.reshape(heads, 2, -1, d_model), rank, nope)
        gw_q = gwq.reshape(heads, qk_dim, d_model).transpose(2, 0, 1)
        return y_loc, dx_loc, gw_q, gw_dkv, gg_kv, gw_kr.T, gw_uk, gw_uv, gwo.reshape(heads, v_dim, d_model)

    return jax.shard_map(block, mesh=mesh, in_specs=(row_spec, row_spec) + (P(),) * 7, out_specs=(row_spec, row_spec) + (per_group,) * 7, check_vma=False)
```

```python
import functools

import jax
import jax.numpy as jnp
import numpy as np
from jax import lax
from jax.experimental import pallas as pl
from jax.experimental.pallas import tpu as pltpu
from jax.sharding import PartitionSpec as P


ROPE_THETA = 10000.0
NORM_EPS = 1e-6
LOG2E = 1.4426950408889634
MASKED = -1e30
F32 = jnp.float32
BF16 = jnp.bfloat16
OVER_ROWS = (((0,), (0,)), ((), ()))
OVER_COLS = (((1,), (1,)), ((), ()))
LANES = 128
SLOT = 2 * LANES
VMEM_LIMIT = 63 * 1024 * 1024
EVENTS = 36


def compiler_params(**more):
    return pltpu.CompilerParams(vmem_limit_bytes=VMEM_LIMIT, **more)


def cost(flops, bytes_accessed=0, transcendentals=0):
    return pl.CostEstimate(flops=int(flops), bytes_accessed=bytes_accessed, transcendentals=transcendentals)


def struct(shape, dtype=F32):
    return jax.ShapeDtypeStruct(shape, dtype)


def whole(*shape):
    return pl.BlockSpec(shape, lambda *i: (0,) * len(shape))


def rows(count, width):
    return pl.BlockSpec((count, width), lambda i, *_: (i, 0))


def zero(*refs):
    for ref in refs:
        ref[...] = jnp.zeros(ref.shape, ref.dtype)


def exact(a, b):
    return jnp.dot(a, b, preferred_element_type=F32)


def over_rows(a, b):
    return lax.dot_general(a, b, OVER_ROWS, preferred_element_type=F32)


def over_cols(a, b):
    return lax.dot_general(a, b, OVER_COLS, preferred_element_type=F32)


def at_block(index, size):
    return pl.ds(pl.multiple_of(index * size, size), size)


def rope_tables(positions, rope_dim, xp=jnp):
    half_dim = rope_dim // 2
    inv_freq = ROPE_THETA ** (-(xp.arange(half_dim, dtype=xp.float32) * 2.0 / rope_dim))
    angles = positions[:, None] * inv_freq[None, :]
    return xp.cos(angles), xp.sin(angles)


def rope_back(g_in, cos_t, sin_t):
    first_half, second_half = jnp.split(g_in, 2, axis=-1)
    return jnp.concatenate([first_half * cos_t + second_half * sin_t, second_half * cos_t - first_half * sin_t], axis=-1)


def attn_kernel(scale, shard, half, nope, rope, place_ref, x_ref, far_ref, near_ref, w_ref, wq_ref, wr_ref, gain_ref, uk_ref, uv_ref, g_ref,
                odq_ref, sent_ref, keep_ref, give_ref, latent_ref,
                w2_ref, wkv_ref, q_ref, k_ref, v_ref, cm_ref, sm_ref, s_ref, m_ref, l_ref, do_ref, d_ref, acc_ref, dk_ref, dv_ref):
    i = pl.program_id(0)
    n = pl.num_programs(0)
    core = place_ref[0]
    bq = q_ref.shape[0]
    bk = x_ref.shape[0]
    vd = v_ref.shape[1]
    rep = bk // LANES

    def keys(j):
        return at_block(j, bk)

    def wide(x):
        return jnp.concatenate([x] * rep, axis=1)

    def fold(x, op):
        return functools.reduce(op, jnp.split(x, rep, axis=1))

    def swapped(t):
        lane = lax.broadcasted_iota(jnp.int32, t.shape, 1)
        return jnp.where(lane % rope < rope // 2, pltpu.roll(t, LANES - rope // 2, 1), pltpu.roll(t, rope // 2, 1))

    def both_tables(t):
        first = lax.broadcasted_iota(jnp.int32, t.shape, 1) < rope
        other = pltpu.roll(t, rope, 1)
        return jnp.where(first, t, other), jnp.where(first, other, t)

    def spread(ref, column):
        ref[...] = jnp.broadcast_to(column, ref.shape)

    @pl.when(i == 0)
    def _():
        w2_ref[...] = jnp.concatenate([wq_ref[0], wr_ref[...]], axis=0).T
        wkv_ref[:, :nope] = uk_ref[...]
        wkv_ref[:, nope:] = uv_ref[...]
        zero(dk_ref, dv_ref)

    step = near_ref.shape[0]

    def project(b, _):
        r = at_block(b, step)
        t = at_block(i * (bk // step) + b, step)
        x = x_ref[r, :]
        c = exact(x, w_ref[...])
        inv = lax.rsqrt(jnp.sum(c * c, axis=1, keepdims=True) * (1.0 / c.shape[1]) + NORM_EPS)
        latent = (c * inv * gain_ref[...]).astype(BF16)
        latent_ref[r, :] = latent
        kv = exact(latent, wkv_ref[...])
        v_ref[t, :] = kv[:, nope:].astype(BF16)
        qk = exact(x, w2_ref[...])
        far = far_ref[pl.ds(i * (bk // step) + b, 1), :]
        lane = lax.broadcasted_iota(jnp.int32, (step, LANES), 1)
        (cos_a, sin_a), (cos_b, sin_b) = both_tables(far), both_tables(near_ref[...])
        cos_t = cos_a * cos_b - sin_a * sin_b
        sin_t = sin_a * cos_b + cos_a * sin_b
        sin_t = jnp.where(lane % rope < rope // 2, -sin_t, sin_t)
        turned = qk[:, nope:]
        turned = turned * cos_t + swapped(turned) * sin_t
        k_ref[t, :] = jnp.concatenate([kv[:, :nope], jnp.where(lane < rope, pltpu.roll(turned, rope, 1), 0.0)], axis=1).astype(BF16)
        q = jnp.concatenate([qk[:, :nope], jnp.where(lane < rope, turned, 0.0)], axis=1).astype(BF16)
        for a in range(step // shard):
            to = at_block(b * (step // shard) + a, half)
            lo, hi = slice(a * shard, a * shard + half), slice(a * shard + half, (a + 1) * shard)
            for ref, value in ((q_ref, q), (cm_ref, cos_t), (sm_ref, sin_t)):
                ref[to, :] = jnp.where(core == 0, value[lo], value[hi])
        return 0

    lax.fori_loop(0, bk // step, project, 0)

    m_ref[...] = jnp.full(m_ref.shape, MASKED, F32)

    def scores(j):
        return over_cols(q_ref[...], k_ref[keys(j), :])

    def note(j, s):
        s_ref[:, keys(j)] = s
        m_ref[...] = jnp.maximum(m_ref[...], fold(s, jnp.maximum))

    def full_tile(j, _):
        note(j, scores(j))
        return 0

    lax.fori_loop(0, i, full_tile, 0)
    row = lax.broadcasted_iota(jnp.int32, (bq, bk), 0)
    col = lax.broadcasted_iota(jnp.int32, (bq, bk), 1)
    note(i, jnp.where(col <= (row // half) * shard + core * half + row % half, scores(i), MASKED))

    spread(m_ref, jnp.max(m_ref[...], axis=1, keepdims=True))
    zero(l_ref, acc_ref)

    def prob_tile(j, _):
        r = keys(j)
        p = jnp.exp2((s_ref[:, r] - wide(m_ref[...])) * (scale * LOG2E))
        s_ref[:, r] = p
        l_ref[...] += fold(p, jnp.add)
        acc_ref[:, :vd] += exact(p.astype(BF16), v_ref[r, :])
        return 0

    lax.fori_loop(0, i + 1, prob_tile, 0)

    inv = 1.0 / jnp.sum(l_ref[...], axis=1, keepdims=True)
    o = acc_ref[:, :vd] * inv
    odq_ref[:, :vd] = o.astype(BF16)
    do = g_ref[...].astype(F32)
    spread(d_ref, jnp.sum(do * o, axis=1, keepdims=True) * inv)
    do_ref[...] = (do * inv).astype(BF16)
    zero(acc_ref)

    def back_tile(j, _):
        r = keys(j)
        p = s_ref[:, r]
        dp = over_cols(do_ref[...], v_ref[r, :])
        ds = (p * (dp - wide(d_ref[...]))).astype(BF16)
        dv_ref[r, :] += over_rows(p.astype(BF16), do_ref[...])
        dk_ref[r, :] += over_rows(ds, q_ref[...])
        acc_ref[...] += exact(ds, k_ref[r, :])
        return 0

    lax.fori_loop(0, i + 1, back_tile, 0)
    dq = acc_ref[...] * scale
    turned = dq[:, nope:]
    turned = turned * cm_ref[...] - swapped(turned) * sm_ref[...]
    odq_ref[:, vd:vd + nope] = dq[:, :nope].astype(BF16)
    odq_ref[:, vd + nope:] = turned.astype(BF16)
    sent_ref[:, :half] = o.astype(BF16).reshape(-1, half, LANES)
    sent_ref[:, half:2 * half] = dq[:, :nope].astype(BF16).reshape(-1, half, LANES)
    turned = turned.reshape(-1, half, LANES)
    low, high = turned[:, :half // 2], turned[:, half // 2:]
    lane = lax.broadcasted_iota(jnp.int32, low.shape, 2)
    sent_ref[:, 2 * half:] = jnp.where(lane < rope, low, pltpu.roll(high, rope, 2)).astype(BF16)

    @pl.when(i == n - 1)
    def _():
        def finish(s, _):
            to = at_block(s, half)
            for ref, side in ((keep_ref, core), (give_ref, 1 - core)):
                r = at_block(2 * s + side, half)
                ref[to, :SLOT] = dk_ref[r, :] * scale
                ref[to, SLOT:] = dv_ref[r, :]
            return 0

        lax.fori_loop(0, dk_ref.shape[0] // shard, finish, 0)


def attention(place, x, far, near, w_dkv, wq, wr, gain, uk, uv, g, scale, shard, nope, rope, n):
    seq, d_model = x.shape
    rank, vd = w_dkv.shape[1], g.shape[1]
    half, nq, bk = shard // 2, seq // 2, seq // n
    bq = nq // n
    sent = seq // shard, 2 * half + half // 2, LANES
    vmem = lambda *shape: pltpu.VMEM(shape, F32)
    packed = lambda *shape: pltpu.VMEM(shape, BF16)
    return pl.pallas_call(
        functools.partial(attn_kernel, scale, shard, half, nope, rope),
        grid_spec=pltpu.PrefetchScalarGridSpec(
            num_scalar_prefetch=1, grid=(n,),
            in_specs=[rows(bk, d_model), whole(*far.shape), whole(*near.shape), whole(*w_dkv.shape), pl.BlockSpec((1, *wq.shape[1:]), lambda i, c: (c[1], 0, 0)),
                      whole(*wr.shape), whole(*gain.shape), whole(*uk.shape), whole(*uv.shape), rows(bq, vd)],
            out_specs=[rows(bq, vd + SLOT), pl.BlockSpec((sent[0] // n, *sent[1:]), lambda i, c: (i, 0, 0)), whole(nq, SLOT + vd), whole(nq, SLOT + vd), rows(bk, rank)],
            scratch_shapes=[packed(d_model, SLOT), packed(rank, nope + vd), packed(bq, SLOT), packed(seq, SLOT), packed(seq, vd),
                            vmem(bq, LANES), vmem(bq, LANES), vmem(bq, seq), vmem(bq, LANES), vmem(bq, LANES), packed(bq, vd), vmem(bq, LANES), vmem(bq, SLOT),
                            vmem(seq, SLOT), vmem(seq, vd)]),
        out_shape=[struct((nq, vd + SLOT), BF16), struct(sent, BF16), struct((nq, SLOT + vd)), struct((nq, SLOT + vd)), struct((seq, rank), BF16)],
        compiler_params=compiler_params(),
        cost_estimate=cost(2 * seq * d_model * (rank + SLOT) + 7 * nq * seq * SLOT, 2 * x.size, nq * seq),
    )(place, x, far, near, w_dkv, wq, wr, gain, uk, uv, g)


def ring_kernel(side, counts, make, n_given, n_made, *refs):
    n_ring, n_each, _ = counts
    total = sum(counts)
    given = refs[:n_given]
    srcs, outs = refs[n_given:n_given + total], refs[n_given + total:n_given + 2 * total + n_made]
    send_sem, recv_sem, own_sem, *rest = refs[n_given + 2 * total + n_made:]
    direct_sem, made = rest[:2], rest[2:]
    sent_to = [(srcs[k], outs[k], k < n_ring + n_each) for k in range(n_ring, total)]
    if make:
        sent_to.append((made[0], outs[total], True))
    n_dev = 2 * side * side
    me = lax.axis_index("cp")
    pos = ((me // 2) % side, me // (2 * side))
    mesh_id = pl.DeviceIdType.MESH

    def at(dx, dy):
        return (lax.rem(pos[1] + dy + side, side) * side + lax.rem(pos[0] + dx + side, side)) * 2 + me % 2

    def shifted(color, first, second):
        return at(second, first) if color else at(first, second)

    sibling = me + 1 - 2 * (me % 2)
    direct = len(sent_to) > 0
    neighbours = [shifted(color, d, 0) for color in range(2) for d in (1, -1)]
    barrier = pltpu.get_barrier_semaphore()

    def greet(peer):
        pl.semaphore_signal(barrier, inc=1, device_id={"cp": peer}, device_id_type=mesh_id)

    def others(do):
        def body(d, _):
            do(d)
            return 0

        lax.fori_loop(1, n_dev, body, 0)

    if direct:
        others(lambda d: greet(me ^ d))
        pl.semaphore_wait(barrier, n_dev - 1)
    else:
        for peer in (*neighbours, sibling):
            greet(peer)
        pl.semaphore_wait(barrier, len(neighbours) + 1)

    def part(ref, color, piece=0, pieces=1):
        size = ref.shape[0] // (2 * pieces)
        return ref.at[pl.ds((pieces * color + piece) * size, size)]

    def copy(src, dst, sems, peer):
        return pltpu.make_async_remote_copy(src_ref=src, dst_ref=dst, send_sem=sems[0], recv_sem=sems[1], device_id={"cp": peer}, device_id_type=mesh_id)

    def sems(k, color, event):
        return send_sem.at[k, color, event], recv_sem.at[k, color, event]

    pending = []

    def send(color, event, block, peer, *piece):
        for k in range(n_ring):
            src, dst = (srcs[k], outs[k].at[me]) if block is None else (outs[k].at[block],) * 2
            pending.append(copy(part(src, color, *piece), part(dst, color, *piece), sems(k, color, event), peer))
            pending[-1].start()

    def arrived(color, event, block, *piece):
        for k in range(n_ring):
            ref = part(outs[k].at[block], color, *piece)
            copy(ref, ref, sems(k, color, event), sibling).wait_recv()

    local = lambda src, dst, k: pltpu.make_async_copy(src, dst, own_sem.at[k])
    own = [local(srcs[k], outs[k].at[me], k) for k in range(n_ring)]
    late = [local(src.at[me] if each else src, dst.at[me], n_ring + k) for k, (src, dst, each) in enumerate(sent_to)]
    late += [local(made[k], outs[total + k], total + k) for k in range(1, n_made)]

    def straight(d):
        for k, (src, dst, each) in enumerate(sent_to):
            yield copy(src.at[me ^ d] if each else src, dst.at[me], [s.at[k, d] for s in direct_sem], me ^ d)

    def start_direct():
        for c in late:
            c.start()
        if direct:
            others(lambda d: [c.start() for c in straight(d)])

    def wait_all():
        for c in own + late:
            c.wait()
        if direct:
            others(lambda d: [c.wait() for c in straight(d)])

    for c in own:
        c.start()
    if not make:
        start_direct()
    finish = make(*given, *made) if make else None

    colors = range(2)
    offsets = (0, -1, 1, 2)
    first_out, relays, second_out, to_sibling, column = 0, 2, 4, 20, 24

    def spread(c, j, block):
        for d, way in enumerate((1, -1)):
            send(c, second_out + 4 * j + d, block, shifted(c, 0, way))
        send(c, to_sibling + j, block, sibling)

    def relay(c, j):
        for d, way in enumerate((1, -1)):
            block = shifted(c, offsets[j], -way)
            arrived(c, second_out + 4 * j + d, block)
            send(c, second_out + relays + 4 * j + d, block, shifted(c, 0, way), d, 2)
            send(c, column + 3 * j + d, block, sibling)

    if not n_ring:
        wait_all()
        return
    for c in colors:
        for d, way in enumerate((1, -1)):
            send(c, first_out + d, None, shifted(c, way, 0))
        spread(c, 0, None)
    for c in colors:
        for d, way in enumerate((1, -1)):
            block = shifted(c, -way, 0)
            arrived(c, first_out + d, block)
            send(c, relays + d, block, shifted(c, way, 0), d, 2)
            spread(c, 1 + d, block)
    for c in colors:
        relay(c, 0)
    if make:
        finish()
    for c in colors:
        across = shifted(c, 2, 0)
        for d in range(2):
            arrived(c, relays + d, across, d, 2)
        spread(c, 3, across)
    if make:
        start_direct()
    for j in range(1, 4):
        for c in colors:
            relay(c, j)
    for j in range(4):
        for c in colors:
            across = shifted(c, offsets[j], 2)
            for d in range(2):
                arrived(c, second_out + relays + 4 * j + d, across, d, 2)
            send(c, column + 2 + 3 * j, across, sibling)
    other = sibling - me
    for c in colors:
        for j in range(4):
            arrived(c, to_sibling + j, shifted(c, offsets[j], 0) + other)
            for d in range(3):
                arrived(c, column + 3 * j + d, shifted(c, offsets[j], offsets[1 + d]) + other)
    for c in pending:
        c.wait_send()
    wait_all()


def ring_gather(n_dev, cid, ring, each=(), same=(), make=None, given=(), made=(), scratch=()):
    side = round((n_dev // 2) ** 0.5)
    sent = [*ring, *each, *same]
    n_made = len(made)
    shapes = [struct(a.shape if len(ring) <= k < len(ring) + len(each) else (n_dev,) + a.shape, a.dtype) for k, a in enumerate(sent)]
    shapes += [struct(a.shape, a.dtype) for a in made]
    counts = len(ring), len(each), len(same)
    n_direct = sum(counts[1:]) + (1 if make else 0)
    dma = pltpu.SemaphoreType.DMA
    in_vmem, anywhere = pl.BlockSpec(memory_space=pltpu.VMEM), pl.BlockSpec(memory_space=pl.ANY)
    return pl.pallas_call(
        functools.partial(ring_kernel, side, counts, make, len(given), n_made),
        in_specs=[anywhere] * len(given) + [in_vmem] * len(sent), out_specs=[anywhere] * len(shapes), out_shape=shapes,
        scratch_shapes=[dma((max(len(ring), 1), 2, EVENTS))] * 2 + [dma((len(shapes),))] + [dma((max(n_direct, 1), n_dev))] * 2 + [*made, *scratch],
        compiler_params=compiler_params(collective_id=cid, has_side_effects=True),
        cost_estimate=cost(4e10),
    )(*given, *sent)


def make_early(gy_ref, w_ref, uk_ref, uv_ref, blocks_ref, uk_head_ref, uv_head_ref, *rest):
    *vmem, sems = rest
    reads = [pltpu.make_async_copy(src, dst, sems.at[k]) for k, (src, dst) in enumerate(zip((gy_ref, w_ref, uk_ref, uv_ref), vmem))]
    for c in reads:
        c.start()
    gy_vmem, w_vmem, uk_vmem, uv_vmem = vmem

    def compute():
        for c in reads:
            c.wait()
        heads, v_dim = w_ref.shape[:2]
        half = blocks_ref.shape[1]
        head = lax.axis_index("cp") // 2

        def two_heads(b, _):
            w = w_vmem[pl.ds(2 * b, 2)].reshape(2 * v_dim, -1)
            g = over_cols(gy_vmem[...], w).astype(BF16)
            for h in range(2):
                for core in range(2):
                    blocks_ref[4 * b + 2 * h + core] = g[core * half:(core + 1) * half, h * v_dim:(h + 1) * v_dim]
            return 0

        lax.fori_loop(0, heads // 2, two_heads, 0)

        def pick(b, _):
            r = at_block(b, LANES)
            for src, dst in ((uk_vmem, uk_head_ref), (uv_vmem, uv_head_ref)):
                w = src[r].astype(F32)
                dst[r, :] = jnp.sum(jnp.where(lax.broadcasted_iota(jnp.int32, w.shape, 1) == head, w, 0.0), axis=1).astype(BF16)
            return 0

        lax.fori_loop(0, uk_head_ref.shape[0] // LANES, pick, 0)

    return compute


def query_grads_kernel(qk_dim, core_ref, x_ref, odq_ref, keep_ref, give_ref, q_acc):
    i = pl.program_id(0)
    core = core_ref[0]
    d_model = x_ref.shape[-1]

    @pl.when(i == 0)
    def _():
        zero(q_acc)

    x = x_ref[...].reshape(-1, d_model)
    dq_t = odq_ref[...].T[-SLOT:][:qk_dim]
    for c in range(4):
        cols = slice(c * d_model // 4, (c + 1) * d_model // 4)
        q_acc[:, cols] += exact(dq_t, x[:, cols])

    @pl.when(i == pl.num_programs(0) - 1)
    def _():
        for ref, side in ((keep_ref, core), (give_ref, 1 - core)):
            ref[...] = q_acc[at_block(side, qk_dim // 2), :]


def output_grads_kernel(core_ref, gy_ref, odq_ref, keep_ref, give_ref, o_acc):
    i = pl.program_id(0)
    core = core_ref[0]
    vd, d_model = o_acc.shape

    @pl.when(i == 0)
    def _():
        zero(o_acc)

    gy = gy_ref[...].reshape(-1, d_model)
    o_t = odq_ref[...].T[:vd]
    for c in range(4):
        cols = slice(c * d_model // 4, (c + 1) * d_model // 4)
        o_acc[:, cols] += exact(o_t, gy[:, cols])

    @pl.when(i == pl.num_programs(0) - 1)
    def _():
        for ref, side in ((keep_ref, core), (give_ref, 1 - core)):
            ref[...] = o_acc[at_block(side, vd // 2), :]


def head_grads(kernel, core, act, odq, n_dev, half, width):
    n = 4
    shards = n_dev // n
    d_model = act.shape[1]
    out = width // 2, d_model
    return pl.pallas_call(
        kernel,
        grid_spec=pltpu.PrefetchScalarGridSpec(
            num_scalar_prefetch=1, grid=(n,),
            in_specs=[pl.BlockSpec((shards, 1, half, d_model), lambda i, c: (i, c[0], 0, 0)), rows(shards * half, odq.shape[1])],
            out_specs=[whole(*out)] * 2, scratch_shapes=[pltpu.VMEM((width, d_model), F32)]),
        out_shape=[struct(out)] * 2, compiler_params=compiler_params(), cost_estimate=cost(act.size * width, act.size),
    )(core[None], act.reshape(n_dev, 2, half, d_model), odq)


def up_grads_kernel(core_ref, latent_ref, kv_ref, keep_ref, give_ref):
    core = core_ref[0]
    up = over_rows(latent_ref[...].reshape(-1, latent_ref.shape[-1]), kv_ref[...])
    count = keep_ref.shape[0]
    width = up.shape[1]
    blocks = keep_ref.shape[1] // width
    for a in range(blocks):
        lo, hi = (up[(s * blocks + a) * count:(s * blocks + a + 1) * count] for s in range(2))
        cols = slice(a * width, (a + 1) * width)
        keep_ref[:, cols] = jnp.where(core == 0, lo, hi)
        give_ref[:, cols] = jnp.where(core == 0, hi, lo)


def up_grads(core, latent, kv, d_model, n_dev, half):
    rank, width = latent.shape[1], kv.shape[1]
    out = rank * width // (2 * d_model), d_model
    return pl.pallas_call(
        up_grads_kernel,
        grid_spec=pltpu.PrefetchScalarGridSpec(
            num_scalar_prefetch=1, grid=(1,),
            in_specs=[pl.BlockSpec((n_dev, 1, half, rank), lambda i, c: (0, c[0], 0, 0)), whole(*kv.shape)], out_specs=[whole(*out)] * 2),
        out_shape=[struct(out)] * 2, compiler_params=compiler_params(), cost_estimate=cost(2 * kv.size * rank, latent.size),
    )(core[None], latent.reshape(n_dev, 2, half, rank), kv)


def finish_kernel(x_ref, low_ref, g_ref, dkv_ref, kr_ref, copy_ref, low_t):
    @pl.when(pl.program_id(0) == 0)
    def _():
        n_dev, _, shard = low_ref.shape
        for d in range(n_dev):
            low_t[:, d * shard:(d + 1) * shard] = low_ref[d]

    g = exact(low_t[...], x_ref[...])
    rank = dkv_ref.shape[1]
    dkv_ref[...] = g[:rank].T
    kr_ref[...] = g[rank:]
    copy_ref[...] = g_ref[...]


def finish(x, low, g, rank):
    seq, d_model = x.shape
    width = low.shape[1]
    rope = width - rank
    steps = 4
    cols = d_model // steps
    piece = rows(g.shape[0] // steps, g.shape[1])
    return pl.pallas_call(
        finish_kernel, grid=(steps,),
        in_specs=[pl.BlockSpec((seq, cols), lambda i: (0, i)), whole(*low.shape), piece],
        out_specs=[rows(cols, rank), pl.BlockSpec((rope, cols), lambda i: (0, i)), piece],
        out_shape=[struct((d_model, rank)), struct((rope, d_model)), struct(g.shape)],
        scratch_shapes=[pltpu.VMEM((width, seq), BF16)],
        compiler_params=compiler_params(), cost_estimate=cost(2 * x.size * width, 2 * x.size + 8 * g.size),
    )(x, low, g)


def spread_heads_kernel(up_ref, uk_ref, uv_ref):
    heads, _, count, cols = up_ref.shape
    for a, block in enumerate(jnp.split(up_ref[...].reshape(heads, count, cols), cols // SLOT, axis=2)):
        for ref, value in zip((uk_ref, uv_ref), jnp.split(block, 2, axis=2)):
            ref[a * count:(a + 1) * count] = jnp.swapaxes(value, 0, 1)


def spread_heads(up, rank, width):
    heads, _, count, cols = up.shape
    steps = 2
    return pl.pallas_call(
        spread_heads_kernel, grid=(2, steps),
        in_specs=[pl.BlockSpec((heads, 1, count, cols // steps), lambda s, a: (0, s, 0, a))],
        out_specs=[pl.BlockSpec((rank // (2 * steps), heads, width), lambda s, a: (s * steps + a, 0, 0))] * 2,
        out_shape=[struct((rank, heads, width))] * 2, compiler_params=compiler_params(), cost_estimate=cost(1e9, 8 * up.size),
    )(up)


def solution(mesh):
    n_dev = mesh.shape['cp']
    row_spec, per_group = P(('dp', 'cp')), P('dp')
    siblings = [(i, i ^ 1) for i in range(n_dev)]

    def block(x_loc, gy_loc, w_q, w_dkv, g_kv, w_kr, w_uk, w_uv, w_o):
        shard, d_model = x_loc.shape
        heads, qk_dim = w_q.shape[1:]
        rank, _, nope = w_uk.shape
        v_dim, rope = w_uv.shape[2], w_kr.shape[1]
        half, seq = shard // 2, n_dev * shard
        me = lax.axis_index('cp')
        head, core = me // 2, me % 2

        def gather(a):
            return lax.all_gather(a, 'cp', axis=0, tiled=True)

        def summed(keep, give):
            return keep + lax.ppermute(give, 'cp', siblings)

        packed = lambda *shape: pltpu.VMEM(shape, BF16)
        given = gy_loc, w_o, w_uk, w_uv
        x_all, d_out, uk, uv = ring_gather(n_dev, 1, [x_loc], make=make_early, given=given, made=(packed(n_dev, half, v_dim), packed(rank, nope), packed(rank, v_dim)),
                                           scratch=[*(packed(*a.shape) for a in given), pltpu.SemaphoreType.DMA((len(given),))])
        x_all, d_out = x_all.reshape(seq, d_model), d_out.reshape(seq // 2, v_dim)
        gy_all = gather(lax.optimization_barrier((gy_loc, x_all))[0])


        def table(positions):
            return np.concatenate([t for t in rope_tables(positions.astype(np.float32), rope, np) for _ in range(LANES // rope)], axis=1)

        far, near = table(np.arange(0, seq, 4 * shard)), table(np.arange(4 * shard))
        gain = g_kv.astype(F32)[None]
        odq, sent, kv_keep, kv_give, latent = attention(jnp.stack([core, head]), x_all, far, near, w_dkv, w_q.transpose(1, 2, 0), w_kr.T, gain, uk, uv, d_out, qk_dim ** -0.5, shard, nope, rope, 4)

        def exchange(a):
            return lax.all_to_all(a, 'cp', 0, 0, tiled=True).reshape(heads, 2, *a.shape[1:])

        q_keep, q_give = head_grads(functools.partial(query_grads_kernel, qk_dim), core, x_all, odq, n_dev, half, qk_dim)
        got_odq = exchange(lax.optimization_barrier((sent, q_keep))[0])
        q_my = summed(q_keep, q_give)
        gwq = gather(q_my)

        kv_sum = lax.optimization_barrier((summed(kv_keep, kv_give), q_keep))[0]
        kv_my = jnp.concatenate([kv_sum[:, :nope], kv_sum[:, SLOT:]], axis=1).astype(BF16)
        dkr_my = kv_sum[:, nope:qk_dim].reshape(n_dev, half * rope // LANES, LANES)
        o_keep, o_give = head_grads(output_grads_kernel, core, gy_all, odq, n_dev, half, v_dim)
        o_my = summed(o_keep, o_give)
        gwo = gather(o_my)
        got_odq, kv_my, _ = lax.optimization_barrier((got_odq, kv_my, o_keep))
        got_kv = exchange(kv_my.reshape(n_dev, half, -1))
        up_keep, up_give = up_grads(core, latent, kv_my, d_model, n_dev, half)
        up_my = summed(up_keep, up_give)
        o_loc, dq_loc, dq_rope = jnp.split(got_odq, [half, 2 * half], axis=2)
        dq_loc = jnp.concatenate([dq_loc, jnp.concatenate([dq_rope[..., :rope], dq_rope[..., rope:]], axis=2)], axis=3)
        o_loc, dq_loc = o_loc.reshape(heads, shard, -1), dq_loc.reshape(heads, shard, -1)
        y_loc = jnp.einsum('htv,hvd->td', o_loc, w_o, preferred_element_type=F32).astype(BF16)
        dx_loc = jnp.einsum('hte,dhe->td', dq_loc, w_q, preferred_element_type=F32)
        dkr_my, y_loc, dx_loc, _, _ = lax.optimization_barrier((dkr_my, y_loc, dx_loc, o_my, up_my))
        got_r, = ring_gather(n_dev, 2, [], [dkr_my])
        got_kv, got_r = lax.optimization_barrier((got_kv, got_r))
        dkr_loc = jnp.sum(got_r.reshape(heads, shard, rope), axis=0)
        dk_loc, dv_loc = jnp.split(got_kv.reshape(heads, shard, -1), [nope], axis=2)
        d_latent = jnp.einsum('htn,chn->tc', dk_loc, w_uk, preferred_element_type=F32) + jnp.einsum('htv,chv->tc', dv_loc, w_uv, preferred_element_type=F32)
        c_loc = exact(x_loc, w_dkv)
        inv_loc = lax.rsqrt(jnp.mean(c_loc * c_loc, axis=-1, keepdims=True) + NORM_EPS)
        c_norm = c_loc * inv_loc
        gg_part = jnp.sum(d_latent * c_norm, axis=0)
        d_norm = d_latent * gain
        dc_loc = (inv_loc * (d_norm - c_norm * jnp.mean(d_norm * c_norm, axis=-1, keepdims=True))).astype(BF16)
        cos_t, sin_t = rope_tables((me * shard + jnp.arange(shard)).astype(F32), rope)
        dkr_raw = rope_back(dkr_loc, cos_t, sin_t).astype(BF16)
        dx_loc = dx_loc + jnp.einsum('tc,dc->td', dc_loc, w_dkv, preferred_element_type=F32) + jnp.einsum('tr,dr->td', dkr_raw, w_kr, preferred_element_type=F32)

        gg_rows = rank // LANES
        gg_part = jnp.pad(gg_part.reshape(gg_rows, LANES), ((0, 8 - gg_rows), (0, 0)))
        low_my = jnp.concatenate([dc_loc, dkr_raw], axis=1).T
        low_my, dx_loc = lax.optimization_barrier((low_my, dx_loc.astype(BF16)))
        low, up, gg = ring_gather(n_dev, 3, [low_my, up_my], (), [gg_part])
        gw_dkv, gw_kr, gwq = finish(x_all, low, gwq, rank)
        gg_kv = jnp.sum(gg, axis=0)[:gg_rows].reshape(rank)
        gw_uk, gw_uv = spread_heads(up.reshape(heads, 2, -1, d_model), rank, nope)
        gw_q = gwq.reshape(heads, qk_dim, d_model).transpose(2, 0, 1)
        return y_loc, dx_loc, gw_q, gw_dkv, gg_kv, gw_kr.T, gw_uk, gw_uv, gwo.reshape(heads, v_dim, d_model)

    return jax.shard_map(block, mesh=mesh, in_specs=(row_spec, row_spec) + (P(),) * 7, out_specs=(row_spec, row_spec) + (per_group,) * 7, check_vma=False)
```

```python
import functools

import jax
import jax.numpy as jnp
import numpy as np
from jax import lax
from jax.experimental import pallas as pl
from jax.experimental.pallas import tpu as pltpu
from jax.sharding import PartitionSpec as P


ROPE_THETA = 10000.0
NORM_EPS = 1e-6
LOG2E = 1.4426950408889634
MASKED = -1e30
F32 = jnp.float32
BF16 = jnp.bfloat16
OVER_ROWS = (((0,), (0,)), ((), ()))
OVER_COLS = (((1,), (1,)), ((), ()))
LANES = 128
SLOT = 2 * LANES
VMEM_LIMIT = 63 * 1024 * 1024
EVENTS = 36


def compiler_params(**more):
    return pltpu.CompilerParams(vmem_limit_bytes=VMEM_LIMIT, **more)


def cost(flops, bytes_accessed=0, transcendentals=0):
    return pl.CostEstimate(flops=int(flops), bytes_accessed=bytes_accessed, transcendentals=transcendentals)


def struct(shape, dtype=F32):
    return jax.ShapeDtypeStruct(shape, dtype)


def whole(*shape):
    return pl.BlockSpec(shape, lambda *i: (0,) * len(shape))


def rows(count, width):
    return pl.BlockSpec((count, width), lambda i, *_: (i, 0))


def zero(*refs):
    for ref in refs:
        ref[...] = jnp.zeros(ref.shape, ref.dtype)


def exact(a, b):
    return jnp.dot(a, b, preferred_element_type=F32)


def over_rows(a, b):
    return lax.dot_general(a, b, OVER_ROWS, preferred_element_type=F32)


def over_cols(a, b):
    return lax.dot_general(a, b, OVER_COLS, preferred_element_type=F32)


def at_block(index, size):
    return pl.ds(pl.multiple_of(index * size, size), size)


def rope_tables(positions, rope_dim, xp=jnp):
    half_dim = rope_dim // 2
    inv_freq = ROPE_THETA ** (-(xp.arange(half_dim, dtype=xp.float32) * 2.0 / rope_dim))
    angles = positions[:, None] * inv_freq[None, :]
    return xp.cos(angles), xp.sin(angles)


def rope_back(g_in, cos_t, sin_t):
    first_half, second_half = jnp.split(g_in, 2, axis=-1)
    return jnp.concatenate([first_half * cos_t + second_half * sin_t, second_half * cos_t - first_half * sin_t], axis=-1)


def attn_kernel(scale, shard, half, nope, rope, place_ref, x_ref, far_ref, near_ref, w_ref, wq_ref, wr_ref, gain_ref, uk_ref, uv_ref, g_ref,
                odq_ref, sent_ref, keep_ref, give_ref, latent_ref,
                w2_ref, wkv_ref, q_ref, k_ref, v_ref, cm_ref, sm_ref, s_ref, m_ref, l_ref, do_ref, d_ref, acc_ref, dk_ref, dv_ref):
    i = pl.program_id(0)
    n = pl.num_programs(0)
    core = place_ref[0]
    bq = q_ref.shape[0]
    bk = x_ref.shape[0]
    vd = v_ref.shape[1]
    rep = bk // LANES

    def keys(j):
        return at_block(j, bk)

    def wide(x):
        return jnp.concatenate([x] * rep, axis=1)

    def fold(x, op):
        return functools.reduce(op, jnp.split(x, rep, axis=1))

    def swapped(t):
        lane = lax.broadcasted_iota(jnp.int32, t.shape, 1)
        return jnp.where(lane % rope < rope // 2, pltpu.roll(t, LANES - rope // 2, 1), pltpu.roll(t, rope // 2, 1))

    def both_tables(t):
        first = lax.broadcasted_iota(jnp.int32, t.shape, 1) < rope
        other = pltpu.roll(t, rope, 1)
        return jnp.where(first, t, other), jnp.where(first, other, t)

    def spread(ref, column):
        ref[...] = jnp.broadcast_to(column, ref.shape)

    @pl.when(i == 0)
    def _():
        w2_ref[...] = jnp.concatenate([wq_ref[0], wr_ref[...]], axis=0).T
        wkv_ref[:, :nope] = uk_ref[...]
        wkv_ref[:, nope:] = uv_ref[...]
        zero(dk_ref, dv_ref)

    step = near_ref.shape[0]

    def project(b, _):
        r = at_block(b, step)
        t = at_block(i * (bk // step) + b, step)
        x = x_ref[r, :]
        c = exact(x, w_ref[...])
        inv = lax.rsqrt(jnp.sum(c * c, axis=1, keepdims=True) * (1.0 / c.shape[1]) + NORM_EPS)
        latent = (c * inv * gain_ref[...]).astype(BF16)
        latent_ref[r, :] = latent
        kv = exact(latent, wkv_ref[...])
        v_ref[t, :] = kv[:, nope:].astype(BF16)
        qk = exact(x, w2_ref[...])
        far = far_ref[pl.ds(i * (bk // step) + b, 1), :]
        lane = lax.broadcasted_iota(jnp.int32, (step, LANES), 1)
        (cos_a, sin_a), (cos_b, sin_b) = both_tables(far), both_tables(near_ref[...])
        cos_t = cos_a * cos_b - sin_a * sin_b
        sin_t = sin_a * cos_b + cos_a * sin_b
        sin_t = jnp.where(lane % rope < rope // 2, -sin_t, sin_t)
        turned = qk[:, nope:]
        turned = turned * cos_t + swapped(turned) * sin_t
        k_ref[t, :] = jnp.concatenate([kv[:, :nope], jnp.where(lane < rope, pltpu.roll(turned, rope, 1), 0.0)], axis=1).astype(BF16)
        q = jnp.concatenate([qk[:, :nope], jnp.where(lane < rope, turned, 0.0)], axis=1).astype(BF16)
        for a in range(step // shard):
            to = at_block(b * (step // shard) + a, half)
            lo, hi = slice(a * shard, a * shard + half), slice(a * shard + half, (a + 1) * shard)
            for ref, value in ((q_ref, q), (cm_ref, cos_t), (sm_ref, sin_t)):
                ref[to, :] = jnp.where(core == 0, value[lo], value[hi])
        return 0

    lax.fori_loop(0, bk // step, project, 0)

    m_ref[...] = jnp.full(m_ref.shape, MASKED, F32)

    def scores(j):
        return over_cols(q_ref[...], k_ref[keys(j), :])

    def note(j, s):
        s_ref[:, keys(j)] = s
        m_ref[...] = jnp.maximum(m_ref[...], fold(s, jnp.maximum))

    def full_tile(j, _):
        note(j, scores(j))
        return 0

    lax.fori_loop(0, i, full_tile, 0)
    row = lax.broadcasted_iota(jnp.int32, (bq, bk), 0)
    col = lax.broadcasted_iota(jnp.int32, (bq, bk), 1)
    note(i, jnp.where(col <= (row // half) * shard + core * half + row % half, scores(i), MASKED))

    spread(m_ref, jnp.max(m_ref[...], axis=1, keepdims=True))
    zero(l_ref, acc_ref)

    def prob_tile(j, _):
        r = keys(j)
        p = jnp.exp2((s_ref[:, r] - wide(m_ref[...])) * (scale * LOG2E))
        s_ref[:, r] = p
        l_ref[...] += fold(p, jnp.add)
        acc_ref[:, :vd] += exact(p.astype(BF16), v_ref[r, :])
        return 0

    lax.fori_loop(0, i + 1, prob_tile, 0)

    inv = 1.0 / jnp.sum(l_ref[...], axis=1, keepdims=True)
    o = acc_ref[:, :vd] * inv
    odq_ref[:, :vd] = o.astype(BF16)
    do = g_ref[...].astype(F32)
    spread(d_ref, jnp.sum(do * o, axis=1, keepdims=True) * inv)
    do_ref[...] = (do * inv).astype(BF16)
    zero(acc_ref)

    def back_tile(j, _):
        r = keys(j)
        p = s_ref[:, r]
        dp = over_cols(do_ref[...], v_ref[r, :])
        ds = (p * (dp - wide(d_ref[...]))).astype(BF16)
        dv_ref[r, :] += over_rows(p.astype(BF16), do_ref[...])
        dk_ref[r, :] += over_rows(ds, q_ref[...])
        acc_ref[...] += exact(ds, k_ref[r, :])
        return 0

    lax.fori_loop(0, i + 1, back_tile, 0)
    dq = acc_ref[...] * scale
    turned = dq[:, nope:]
    turned = turned * cm_ref[...] - swapped(turned) * sm_ref[...]
    odq_ref[:, vd:vd + nope] = dq[:, :nope].astype(BF16)
    odq_ref[:, vd + nope:] = turned.astype(BF16)
    sent_ref[:, :half] = o.astype(BF16).reshape(-1, half, LANES)
    sent_ref[:, half:2 * half] = dq[:, :nope].astype(BF16).reshape(-1, half, LANES)
    turned = turned.reshape(-1, half, LANES)
    low, high = turned[:, :half // 2], turned[:, half // 2:]
    lane = lax.broadcasted_iota(jnp.int32, low.shape, 2)
    sent_ref[:, 2 * half:] = jnp.where(lane < rope, low, pltpu.roll(high, rope, 2)).astype(BF16)

    @pl.when(i == n - 1)
    def _():
        def finish(s, _):
            to = at_block(s, half)
            for ref, side in ((keep_ref, core), (give_ref, 1 - core)):
                r = at_block(2 * s + side, half)
                ref[to, :SLOT] = dk_ref[r, :] * scale
                ref[to, SLOT:] = dv_ref[r, :]
            return 0

        lax.fori_loop(0, dk_ref.shape[0] // shard, finish, 0)


def attention(place, x, far, near, w_dkv, wq, wr, gain, uk, uv, g, scale, shard, nope, rope, n):
    seq, d_model = x.shape
    rank, vd = w_dkv.shape[1], g.shape[1]
    half, nq, bk = shard // 2, seq // 2, seq // n
    bq = nq // n
    sent = seq // shard, 2 * half + half // 2, LANES
    vmem = lambda *shape: pltpu.VMEM(shape, F32)
    packed = lambda *shape: pltpu.VMEM(shape, BF16)
    return pl.pallas_call(
        functools.partial(attn_kernel, scale, shard, half, nope, rope),
        grid_spec=pltpu.PrefetchScalarGridSpec(
            num_scalar_prefetch=1, grid=(n,),
            in_specs=[rows(bk, d_model), whole(*far.shape), whole(*near.shape), whole(*w_dkv.shape), pl.BlockSpec((1, *wq.shape[1:]), lambda i, c: (c[1], 0, 0)),
                      whole(*wr.shape), whole(*gain.shape), whole(*uk.shape), whole(*uv.shape), rows(bq, vd)],
            out_specs=[rows(bq, vd + SLOT), pl.BlockSpec((sent[0] // n, *sent[1:]), lambda i, c: (i, 0, 0)), whole(nq, SLOT + vd), whole(nq, SLOT + vd), rows(bk, rank)],
            scratch_shapes=[packed(d_model, SLOT), packed(rank, nope + vd), packed(bq, SLOT), packed(seq, SLOT), packed(seq, vd),
                            vmem(bq, LANES), vmem(bq, LANES), vmem(bq, seq), vmem(bq, LANES), vmem(bq, LANES), packed(bq, vd), vmem(bq, LANES), vmem(bq, SLOT),
                            vmem(seq, SLOT), vmem(seq, vd)]),
        out_shape=[struct((nq, vd + SLOT), BF16), struct(sent, BF16), struct((nq, SLOT + vd)), struct((nq, SLOT + vd)), struct((seq, rank), BF16)],
        compiler_params=compiler_params(),
        cost_estimate=cost(2 * seq * d_model * (rank + SLOT) + 7 * nq * seq * SLOT, 2 * x.size, nq * seq),
    )(place, x, far, near, w_dkv, wq, wr, gain, uk, uv, g)


def ring_kernel(side, counts, make, n_given, n_made, *refs):
    n_ring, n_each, _ = counts
    total = sum(counts)
    given = refs[:n_given]
    srcs, outs = refs[n_given:n_given + total], refs[n_given + total:n_given + 2 * total + n_made]
    send_sem, recv_sem, own_sem, *rest = refs[n_given + 2 * total + n_made:]
    direct_sem, made = rest[:2], rest[2:]
    sent_to = [(srcs[k], outs[k], k < n_ring + n_each) for k in range(n_ring, total)]
    if make:
        sent_to.append((made[0], outs[total], True))
    n_dev = 2 * side * side
    me = lax.axis_index("cp")
    pos = ((me // 2) % side, me // (2 * side))
    mesh_id = pl.DeviceIdType.MESH

    def at(dx, dy):
        return (lax.rem(pos[1] + dy + side, side) * side + lax.rem(pos[0] + dx + side, side)) * 2 + me % 2

    def shifted(color, first, second):
        return at(second, first) if color else at(first, second)

    sibling = me + 1 - 2 * (me % 2)
    direct = len(sent_to) > 0
    neighbours = [shifted(color, d, 0) for color in range(2) for d in (1, -1)]
    barrier = pltpu.get_barrier_semaphore()

    def greet(peer):
        pl.semaphore_signal(barrier, inc=1, device_id={"cp": peer}, device_id_type=mesh_id)

    def others(do):
        def body(d, _):
            do(d)
            return 0

        lax.fori_loop(1, n_dev, body, 0)

    if direct:
        others(lambda d: greet(me ^ d))
        pl.semaphore_wait(barrier, n_dev - 1)
    else:
        for peer in (*neighbours, sibling):
            greet(peer)
        pl.semaphore_wait(barrier, len(neighbours) + 1)

    def part(ref, color, piece=0, pieces=1):
        size = ref.shape[0] // (2 * pieces)
        return ref.at[pl.ds((pieces * color + piece) * size, size)]

    def copy(src, dst, sems, peer):
        return pltpu.make_async_remote_copy(src_ref=src, dst_ref=dst, send_sem=sems[0], recv_sem=sems[1], device_id={"cp": peer}, device_id_type=mesh_id)

    def sems(k, color, event):
        return send_sem.at[k, color, event], recv_sem.at[k, color, event]

    pending = []

    def send(color, event, block, peer, *piece):
        for k in range(n_ring):
            src, dst = (srcs[k], outs[k].at[me]) if block is None else (outs[k].at[block],) * 2
            pending.append(copy(part(src, color, *piece), part(dst, color, *piece), sems(k, color, event), peer))
            pending[-1].start()

    def arrived(color, event, block, *piece):
        for k in range(n_ring):
            ref = part(outs[k].at[block], color, *piece)
            copy(ref, ref, sems(k, color, event), sibling).wait_recv()

    local = lambda src, dst, k: pltpu.make_async_copy(src, dst, own_sem.at[k])
    own = [local(srcs[k], outs[k].at[me], k) for k in range(n_ring)]
    late = [local(src.at[me] if each else src, dst.at[me], n_ring + k) for k, (src, dst, each) in enumerate(sent_to)]
    late += [local(made[k], outs[total + k], total + k) for k in range(1, n_made)]

    def straight(d):
        for k, (src, dst, each) in enumerate(sent_to):
            yield copy(src.at[me ^ d] if each else src, dst.at[me], [s.at[k, d] for s in direct_sem], me ^ d)

    def start_direct():
        for c in late:
            c.start()
        if direct:
            others(lambda d: [c.start() for c in straight(d)])

    def wait_all():
        for c in own + late:
            c.wait()
        if direct:
            others(lambda d: [c.wait() for c in straight(d)])

    for c in own:
        c.start()
    if not make:
        start_direct()
    finish = make(*given, *made) if make else None

    colors = range(2)
    offsets = (0, -1, 1, 2)
    first_out, relays, second_out, to_sibling, column = 0, 2, 4, 20, 24

    def spread(c, j, block):
        for d, way in enumerate((1, -1)):
            send(c, second_out + 4 * j + d, block, shifted(c, 0, way))
        send(c, to_sibling + j, block, sibling)

    def relay(c, j):
        for d, way in enumerate((1, -1)):
            block = shifted(c, offsets[j], -way)
            arrived(c, second_out + 4 * j + d, block)
            send(c, second_out + relays + 4 * j + d, block, shifted(c, 0, way), d, 2)
            send(c, column + 3 * j + d, block, sibling)

    if not n_ring:
        wait_all()
        return
    for c in colors:
        for d, way in enumerate((1, -1)):
            send(c, first_out + d, None, shifted(c, way, 0))
        spread(c, 0, None)
    for c in colors:
        for d, way in enumerate((1, -1)):
            block = shifted(c, -way, 0)
            arrived(c, first_out + d, block)
            send(c, relays + d, block, shifted(c, way, 0), d, 2)
            spread(c, 1 + d, block)
    for c in colors:
        relay(c, 0)
    if make:
        finish()
    for c in colors:
        across = shifted(c, 2, 0)
        for d in range(2):
            arrived(c, relays + d, across, d, 2)
        spread(c, 3, across)
    if make:
        start_direct()
    for j in range(1, 4):
        for c in colors:
            relay(c, j)
    for j in range(4):
        for c in colors:
            across = shifted(c, offsets[j], 2)
            for d in range(2):
                arrived(c, second_out + relays + 4 * j + d, across, d, 2)
            send(c, column + 2 + 3 * j, across, sibling)
    other = sibling - me
    for c in colors:
        for j in range(4):
            arrived(c, to_sibling + j, shifted(c, offsets[j], 0) + other)
            for d in range(3):
                arrived(c, column + 3 * j + d, shifted(c, offsets[j], offsets[1 + d]) + other)
    for c in pending:
        c.wait_send()
    wait_all()


def ring_gather(n_dev, cid, ring, each=(), same=(), make=None, given=(), made=(), scratch=()):
    side = round((n_dev // 2) ** 0.5)
    sent = [*ring, *each, *same]
    n_made = len(made)
    shapes = [struct(a.shape if len(ring) <= k < len(ring) + len(each) else (n_dev,) + a.shape, a.dtype) for k, a in enumerate(sent)]
    shapes += [struct(a.shape, a.dtype) for a in made]
    counts = len(ring), len(each), len(same)
    n_direct = sum(counts[1:]) + (1 if make else 0)
    dma = pltpu.SemaphoreType.DMA
    in_vmem, anywhere = pl.BlockSpec(memory_space=pltpu.VMEM), pl.BlockSpec(memory_space=pl.ANY)
    return pl.pallas_call(
        functools.partial(ring_kernel, side, counts, make, len(given), n_made),
        in_specs=[anywhere] * len(given) + [in_vmem] * len(sent), out_specs=[anywhere] * len(shapes), out_shape=shapes,
        scratch_shapes=[dma((max(len(ring), 1), 2, EVENTS))] * 2 + [dma((len(shapes),))] + [dma((max(n_direct, 1), n_dev))] * 2 + [*made, *scratch],
        compiler_params=compiler_params(collective_id=cid, has_side_effects=True),
        cost_estimate=cost(4e10),
    )(*given, *sent)


def make_early(gy_ref, w_ref, uk_ref, uv_ref, blocks_ref, uk_head_ref, uv_head_ref, *rest):
    *vmem, sems = rest
    reads = [pltpu.make_async_copy(src, dst, sems.at[k]) for k, (src, dst) in enumerate(zip((gy_ref, w_ref, uk_ref, uv_ref), vmem))]
    for c in reads:
        c.start()
    gy_vmem, w_vmem, uk_vmem, uv_vmem = vmem

    def compute():
        for c in reads:
            c.wait()
        heads, v_dim = w_ref.shape[:2]
        half = blocks_ref.shape[1]
        head = lax.axis_index("cp") // 2

        def two_heads(b, _):
            w = w_vmem[pl.ds(2 * b, 2)].reshape(2 * v_dim, -1)
            g = over_cols(gy_vmem[...], w).astype(BF16)
            for h in range(2):
                for core in range(2):
                    blocks_ref[4 * b + 2 * h + core] = g[core * half:(core + 1) * half, h * v_dim:(h + 1) * v_dim]
            return 0

        lax.fori_loop(0, heads // 2, two_heads, 0)

        def pick(b, _):
            r = at_block(b, LANES)
            for src, dst in ((uk_vmem, uk_head_ref), (uv_vmem, uv_head_ref)):
                w = src[r].astype(F32)
                dst[r, :] = jnp.sum(jnp.where(lax.broadcasted_iota(jnp.int32, w.shape, 1) == head, w, 0.0), axis=1).astype(BF16)
            return 0

        lax.fori_loop(0, uk_head_ref.shape[0] // LANES, pick, 0)

    return compute


def query_grads_kernel(qk_dim, core_ref, x_ref, odq_ref, keep_ref, give_ref, q_acc):
    i = pl.program_id(0)
    core = core_ref[0]
    d_model = x_ref.shape[-1]

    @pl.when(i == 0)
    def _():
        zero(q_acc)

    x = x_ref[...].reshape(-1, d_model)
    dq_t = odq_ref[...].T[-SLOT:][:qk_dim]
    for c in range(4):
        cols = slice(c * d_model // 4, (c + 1) * d_model // 4)
        q_acc[:, cols] += exact(dq_t, x[:, cols])

    @pl.when(i == pl.num_programs(0) - 1)
    def _():
        for ref, side in ((keep_ref, core), (give_ref, 1 - core)):
            ref[...] = q_acc[at_block(side, qk_dim // 2), :]


def output_grads_kernel(core_ref, gy_ref, odq_ref, keep_ref, give_ref, o_acc):
    i = pl.program_id(0)
    core = core_ref[0]
    vd, d_model = o_acc.shape

    @pl.when(i == 0)
    def _():
        zero(o_acc)

    gy = gy_ref[...].reshape(-1, d_model)
    o_t = odq_ref[...].T[:vd]
    for c in range(4):
        cols = slice(c * d_model // 4, (c + 1) * d_model // 4)
        o_acc[:, cols] += exact(o_t, gy[:, cols])

    @pl.when(i == pl.num_programs(0) - 1)
    def _():
        for ref, side in ((keep_ref, core), (give_ref, 1 - core)):
            ref[...] = o_acc[at_block(side, vd // 2), :]


def head_grads(kernel, core, act, odq, n_dev, half, width):
    n = 4
    shards = n_dev // n
    d_model = act.shape[1]
    out = width // 2, d_model
    return pl.pallas_call(
        kernel,
        grid_spec=pltpu.PrefetchScalarGridSpec(
            num_scalar_prefetch=1, grid=(n,),
            in_specs=[pl.BlockSpec((shards, 1, half, d_model), lambda i, c: (i, c[0], 0, 0)), rows(shards * half, odq.shape[1])],
            out_specs=[whole(*out)] * 2, scratch_shapes=[pltpu.VMEM((width, d_model), F32)]),
        out_shape=[struct(out)] * 2, compiler_params=compiler_params(), cost_estimate=cost(act.size * width, act.size),
    )(core[None], act.reshape(n_dev, 2, half, d_model), odq)


def up_grads_kernel(core_ref, latent_ref, kv_ref, keep_ref, give_ref):
    core = core_ref[0]
    up = over_rows(latent_ref[...].reshape(-1, latent_ref.shape[-1]), kv_ref[...])
    count = keep_ref.shape[0]
    width = up.shape[1]
    blocks = keep_ref.shape[1] // width
    for a in range(blocks):
        lo, hi = (up[(s * blocks + a) * count:(s * blocks + a + 1) * count] for s in range(2))
        cols = slice(a * width, (a + 1) * width)
        keep_ref[:, cols] = jnp.where(core == 0, lo, hi)
        give_ref[:, cols] = jnp.where(core == 0, hi, lo)


def up_grads(core, latent, kv, d_model, n_dev, half):
    rank, width = latent.shape[1], kv.shape[1]
    out = rank * width // (2 * d_model), d_model
    return pl.pallas_call(
        up_grads_kernel,
        grid_spec=pltpu.PrefetchScalarGridSpec(
            num_scalar_prefetch=1, grid=(1,),
            in_specs=[pl.BlockSpec((n_dev, 1, half, rank), lambda i, c: (0, c[0], 0, 0)), whole(*kv.shape)], out_specs=[whole(*out)] * 2),
        out_shape=[struct(out)] * 2, compiler_params=compiler_params(), cost_estimate=cost(2 * kv.size * rank, latent.size),
    )(core[None], latent.reshape(n_dev, 2, half, rank), kv)


def finish_kernel(x_ref, low_ref, g_ref, dkv_ref, kr_ref, copy_ref, low_t):
    @pl.when(pl.program_id(0) == 0)
    def _():
        n_dev, _, shard = low_ref.shape
        for d in range(n_dev):
            low_t[:, d * shard:(d + 1) * shard] = low_ref[d]

    g = exact(low_t[...], x_ref[...])
    rank = dkv_ref.shape[1]
    dkv_ref[...] = g[:rank].T
    kr_ref[...] = g[rank:]
    copy_ref[...] = g_ref[...]


def finish(x, low, g, rank):
    seq, d_model = x.shape
    width = low.shape[1]
    rope = width - rank
    steps = 4
    cols = d_model // steps
    piece = rows(g.shape[0] // steps, g.shape[1])
    return pl.pallas_call(
        finish_kernel, grid=(steps,),
        in_specs=[pl.BlockSpec((seq, cols), lambda i: (0, i)), whole(*low.shape), piece],
        out_specs=[rows(cols, rank), pl.BlockSpec((rope, cols), lambda i: (0, i)), piece],
        out_shape=[struct((d_model, rank)), struct((rope, d_model)), struct(g.shape)],
        scratch_shapes=[pltpu.VMEM((width, seq), BF16)],
        compiler_params=compiler_params(), cost_estimate=cost(2 * x.size * width, 2 * x.size + 8 * g.size),
    )(x, low, g)


def spread_heads_kernel(up_ref, uk_ref, uv_ref):
    heads, _, count, cols = up_ref.shape
    for a, block in enumerate(jnp.split(up_ref[...].reshape(heads, count, cols), cols // SLOT, axis=2)):
        for ref, value in zip((uk_ref, uv_ref), jnp.split(block, 2, axis=2)):
            ref[a * count:(a + 1) * count] = jnp.swapaxes(value, 0, 1)


def spread_heads(up, rank, width):
    heads, _, count, cols = up.shape
    steps = 2
    return pl.pallas_call(
        spread_heads_kernel, grid=(2, steps),
        in_specs=[pl.BlockSpec((heads, 1, count, cols // steps), lambda s, a: (0, s, 0, a))],
        out_specs=[pl.BlockSpec((rank // (2 * steps), heads, width), lambda s, a: (s * steps + a, 0, 0))] * 2,
        out_shape=[struct((rank, heads, width))] * 2, compiler_params=compiler_params(), cost_estimate=cost(1e9, 8 * up.size),
    )(up)


def solution(mesh):
    n_dev = mesh.shape['cp']
    row_spec, per_group = P(('dp', 'cp')), P('dp')
    siblings = [(i, i ^ 1) for i in range(n_dev)]

    def block(x_loc, gy_loc, w_q, w_dkv, g_kv, w_kr, w_uk, w_uv, w_o):
        shard, d_model = x_loc.shape
        heads, qk_dim = w_q.shape[1:]
        rank, _, nope = w_uk.shape
        v_dim, rope = w_uv.shape[2], w_kr.shape[1]
        half, seq = shard // 2, n_dev * shard
        me = lax.axis_index('cp')
        head, core = me // 2, me % 2

        def gather(a):
            return lax.all_gather(a, 'cp', axis=0, tiled=True)

        def summed(keep, give):
            return keep + lax.ppermute(give, 'cp', siblings)

        packed = lambda *shape: pltpu.VMEM(shape, BF16)
        given = gy_loc, w_o, w_uk, w_uv
        x_all, d_out, uk, uv = ring_gather(n_dev, 1, [x_loc], make=make_early, given=given, made=(packed(n_dev, half, v_dim), packed(rank, nope), packed(rank, v_dim)),
                                           scratch=[*(packed(*a.shape) for a in given), pltpu.SemaphoreType.DMA((len(given),))])
        x_all, d_out = x_all.reshape(seq, d_model), d_out.reshape(seq // 2, v_dim)
        gy_all = gather(lax.optimization_barrier((gy_loc, x_all))[0])


        def table(positions):
            return np.concatenate([t for t in rope_tables(positions.astype(np.float32), rope, np) for _ in range(LANES // rope)], axis=1)

        far, near = table(np.arange(0, seq, 4 * shard)), table(np.arange(4 * shard))
        gain = g_kv.astype(F32)[None]
        odq, sent, kv_keep, kv_give, latent = attention(jnp.stack([core, head]), x_all, far, near, w_dkv, w_q.transpose(1, 2, 0), w_kr.T, gain, uk, uv, d_out, qk_dim ** -0.5, shard, nope, rope, 4)

        def exchange(a):
            return lax.all_to_all(a, 'cp', 0, 0, tiled=True).reshape(heads, 2, *a.shape[1:])

        q_keep, q_give = head_grads(functools.partial(query_grads_kernel, qk_dim), core, x_all, odq, n_dev, half, qk_dim)
        got_odq = exchange(lax.optimization_barrier((sent, q_keep))[0])
        q_my = summed(q_keep, q_give)
        gwq = gather(q_my)

        kv_sum = lax.optimization_barrier((summed(kv_keep, kv_give), q_keep))[0]
        kv_my = jnp.concatenate([kv_sum[:, :nope], kv_sum[:, SLOT:]], axis=1).astype(BF16)
        dkr_my = kv_sum[:, nope:qk_dim].reshape(n_dev, half * rope // LANES, LANES)
        o_keep, o_give = head_grads(output_grads_kernel, core, gy_all, odq, n_dev, half, v_dim)
        o_my = summed(o_keep, o_give)
        gwo = gather(o_my)
        got_odq, kv_my, _ = lax.optimization_barrier((got_odq, kv_my, o_keep))
        got_kv = exchange(kv_my.reshape(n_dev, half, -1))
        up_keep, up_give = up_grads(core, latent, kv_my, d_model, n_dev, half)
        up_my = summed(up_keep, up_give)
        dkr_my, _, _ = lax.optimization_barrier((dkr_my, o_my, up_my))
        got_r, = ring_gather(n_dev, 2, [], [dkr_my])
        got_odq, got_r = lax.optimization_barrier((got_odq, got_r))
        o_loc, dq_loc, dq_rope = jnp.split(got_odq, [half, 2 * half], axis=2)
        dq_loc = jnp.concatenate([dq_loc, jnp.concatenate([dq_rope[..., :rope], dq_rope[..., rope:]], axis=2)], axis=3)
        o_loc, dq_loc = o_loc.reshape(heads, shard, -1), dq_loc.reshape(heads, shard, -1)
        y_loc = jnp.einsum('htv,hvd->td', o_loc, w_o, preferred_element_type=F32).astype(BF16)
        dx_loc = jnp.einsum('hte,dhe->td', dq_loc, w_q, preferred_element_type=F32)
        got_kv, got_r, y_loc, dx_loc = lax.optimization_barrier((got_kv, got_r, y_loc, dx_loc))
        dkr_loc = jnp.sum(got_r.reshape(heads, shard, rope), axis=0)
        dk_loc, dv_loc = jnp.split(got_kv.reshape(heads, shard, -1), [nope], axis=2)
        d_latent = jnp.einsum('htn,chn->tc', dk_loc, w_uk, preferred_element_type=F32) + jnp.einsum('htv,chv->tc', dv_loc, w_uv, preferred_element_type=F32)
        c_loc = exact(x_loc, w_dkv)
        inv_loc = lax.rsqrt(jnp.mean(c_loc * c_loc, axis=-1, keepdims=True) + NORM_EPS)
        c_norm = c_loc * inv_loc
        gg_part = jnp.sum(d_latent * c_norm, axis=0)
        d_norm = d_latent * gain
        dc_loc = (inv_loc * (d_norm - c_norm * jnp.mean(d_norm * c_norm, axis=-1, keepdims=True))).astype(BF16)
        cos_t, sin_t = rope_tables((me * shard + jnp.arange(shard)).astype(F32), rope)
        dkr_raw = rope_back(dkr_loc, cos_t, sin_t).astype(BF16)
        dx_loc = dx_loc + jnp.einsum('tc,dc->td', dc_loc, w_dkv, preferred_element_type=F32) + jnp.einsum('tr,dr->td', dkr_raw, w_kr, preferred_element_type=F32)

        gg_rows = rank // LANES
        gg_part = jnp.pad(gg_part.reshape(gg_rows, LANES), ((0, 8 - gg_rows), (0, 0)))
        low_my = jnp.concatenate([dc_loc, dkr_raw], axis=1).T
        low_my, dx_loc = lax.optimization_barrier((low_my, dx_loc.astype(BF16)))
        low, up, gg = ring_gather(n_dev, 3, [low_my, up_my], (), [gg_part])
        gw_dkv, gw_kr, gwq = finish(x_all, low, gwq, rank)
        gg_kv = jnp.sum(gg, axis=0)[:gg_rows].reshape(rank)
        gw_uk, gw_uv = spread_heads(up.reshape(heads, 2, -1, d_model), rank, nope)
        gw_q = gwq.reshape(heads, qk_dim, d_model).transpose(2, 0, 1)
        return y_loc, dx_loc, gw_q, gw_dkv, gg_kv, gw_kr.T, gw_uk, gw_uv, gwo.reshape(heads, v_dim, d_model)

    return jax.shard_map(block, mesh=mesh, in_specs=(row_spec, row_spec) + (P(),) * 7, out_specs=(row_spec, row_spec) + (per_group,) * 7, check_vma=False)
```

```python
import functools

import jax
import jax.numpy as jnp
import numpy as np
from jax import lax
from jax.experimental import pallas as pl
from jax.experimental.pallas import tpu as pltpu
from jax.sharding import PartitionSpec as P


ROPE_THETA = 10000.0
NORM_EPS = 1e-6
LOG2E = 1.4426950408889634
MASKED = -1e30
F32 = jnp.float32
BF16 = jnp.bfloat16
OVER_ROWS = (((0,), (0,)), ((), ()))
OVER_COLS = (((1,), (1,)), ((), ()))
LANES = 128
SLOT = 2 * LANES
VMEM_LIMIT = 63 * 1024 * 1024
EVENTS = 36


def compiler_params(**more):
    return pltpu.CompilerParams(vmem_limit_bytes=VMEM_LIMIT, **more)


def cost(flops, bytes_accessed=0, transcendentals=0):
    return pl.CostEstimate(flops=int(flops), bytes_accessed=bytes_accessed, transcendentals=transcendentals)


def struct(shape, dtype=F32):
    return jax.ShapeDtypeStruct(shape, dtype)


def whole(*shape):
    return pl.BlockSpec(shape, lambda *i: (0,) * len(shape))


def rows(count, width):
    return pl.BlockSpec((count, width), lambda i, *_: (i, 0))


def zero(*refs):
    for ref in refs:
        ref[...] = jnp.zeros(ref.shape, ref.dtype)


def exact(a, b):
    return jnp.dot(a, b, preferred_element_type=F32)


def over_rows(a, b):
    return lax.dot_general(a, b, OVER_ROWS, preferred_element_type=F32)


def over_cols(a, b):
    return lax.dot_general(a, b, OVER_COLS, preferred_element_type=F32)


def at_block(index, size):
    return pl.ds(pl.multiple_of(index * size, size), size)


def rope_tables(positions, rope_dim, xp=jnp):
    half_dim = rope_dim // 2
    inv_freq = ROPE_THETA ** (-(xp.arange(half_dim, dtype=xp.float32) * 2.0 / rope_dim))
    angles = positions[:, None] * inv_freq[None, :]
    return xp.cos(angles), xp.sin(angles)


def rope_back(g_in, cos_t, sin_t):
    first_half, second_half = jnp.split(g_in, 2, axis=-1)
    return jnp.concatenate([first_half * cos_t + second_half * sin_t, second_half * cos_t - first_half * sin_t], axis=-1)


def attn_kernel(scale, shard, half, nope, rope, place_ref, x_ref, far_ref, near_ref, w_ref, wq_ref, wr_ref, gain_ref, uk_ref, uv_ref, g_ref,
                odq_ref, sent_ref, keep_ref, give_ref, latent_ref,
                w2_ref, wkv_ref, q_ref, k_ref, v_ref, cm_ref, sm_ref, s_ref, m_ref, l_ref, do_ref, d_ref, acc_ref, dk_ref, dv_ref):
    i = pl.program_id(0)
    n = pl.num_programs(0)
    core = place_ref[0]
    bq = q_ref.shape[0]
    bk = x_ref.shape[0]
    vd = v_ref.shape[1]
    rep = bk // LANES

    def keys(j):
        return at_block(j, bk)

    def wide(x):
        return jnp.concatenate([x] * rep, axis=1)

    def fold(x, op):
        return functools.reduce(op, jnp.split(x, rep, axis=1))

    def swapped(t):
        lane = lax.broadcasted_iota(jnp.int32, t.shape, 1)
        return jnp.where(lane % rope < rope // 2, pltpu.roll(t, LANES - rope // 2, 1), pltpu.roll(t, rope // 2, 1))

    def both_tables(t):
        first = lax.broadcasted_iota(jnp.int32, t.shape, 1) < rope
        other = pltpu.roll(t, rope, 1)
        return jnp.where(first, t, other), jnp.where(first, other, t)

    def spread(ref, column):
        ref[...] = jnp.broadcast_to(column, ref.shape)

    @pl.when(i == 0)
    def _():
        w2_ref[...] = jnp.concatenate([wq_ref[0], wr_ref[...]], axis=0).T
        wkv_ref[:, :nope] = uk_ref[...]
        wkv_ref[:, nope:] = uv_ref[...]
        zero(dk_ref, dv_ref)

    step = near_ref.shape[0]

    def project(b, _):
        r = at_block(b, step)
        t = at_block(i * (bk // step) + b, step)
        x = x_ref[r, :]
        c = exact(x, w_ref[...])
        inv = lax.rsqrt(jnp.sum(c * c, axis=1, keepdims=True) * (1.0 / c.shape[1]) + NORM_EPS)
        latent = (c * inv * gain_ref[...]).astype(BF16)
        latent_ref[r, :] = latent
        kv = exact(latent, wkv_ref[...])
        v_ref[t, :] = kv[:, nope:].astype(BF16)
        qk = exact(x, w2_ref[...])
        far = far_ref[pl.ds(i * (bk // step) + b, 1), :]
        lane = lax.broadcasted_iota(jnp.int32, (step, LANES), 1)
        (cos_a, sin_a), (cos_b, sin_b) = both_tables(far), both_tables(near_ref[...])
        cos_t = cos_a * cos_b - sin_a * sin_b
        sin_t = sin_a * cos_b + cos_a * sin_b
        sin_t = jnp.where(lane % rope < rope // 2, -sin_t, sin_t)
        turned = qk[:, nope:]
        turned = turned * cos_t + swapped(turned) * sin_t
        k_ref[t, :] = jnp.concatenate([kv[:, :nope], jnp.where(lane < rope, pltpu.roll(turned, rope, 1), 0.0)], axis=1).astype(BF16)
        q = jnp.concatenate([qk[:, :nope], jnp.where(lane < rope, turned, 0.0)], axis=1).astype(BF16)
        for a in range(step // shard):
            to = at_block(b * (step // shard) + a, half)
            lo, hi = slice(a * shard, a * shard + half), slice(a * shard + half, (a + 1) * shard)
            for ref, value in ((q_ref, q), (cm_ref, cos_t), (sm_ref, sin_t)):
                ref[to, :] = jnp.where(core == 0, value[lo], value[hi])
        return 0

    lax.fori_loop(0, bk // step, project, 0)

    m_ref[...] = jnp.full(m_ref.shape, MASKED, F32)

    def scores(j):
        return over_cols(q_ref[...], k_ref[keys(j), :])

    def note(j, s):
        s_ref[:, keys(j)] = s
        m_ref[...] = jnp.maximum(m_ref[...], fold(s, jnp.maximum))

    def full_tile(j, _):
        note(j, scores(j))
        return 0

    lax.fori_loop(0, i, full_tile, 0)
    row = lax.broadcasted_iota(jnp.int32, (bq, bk), 0)
    col = lax.broadcasted_iota(jnp.int32, (bq, bk), 1)
    note(i, jnp.where(col <= (row // half) * shard + core * half + row % half, scores(i), MASKED))

    spread(m_ref, jnp.max(m_ref[...], axis=1, keepdims=True))
    zero(l_ref, acc_ref)

    def prob_tile(j, _):
        r = keys(j)
        p = jnp.exp2((s_ref[:, r] - wide(m_ref[...])) * (scale * LOG2E))
        s_ref[:, r] = p
        l_ref[...] += fold(p, jnp.add)
        acc_ref[:, :vd] += exact(p.astype(BF16), v_ref[r, :])
        return 0

    lax.fori_loop(0, i + 1, prob_tile, 0)

    inv = 1.0 / jnp.sum(l_ref[...], axis=1, keepdims=True)
    o = acc_ref[:, :vd] * inv
    odq_ref[:, :vd] = o.astype(BF16)
    do = g_ref[...].astype(F32)
    spread(d_ref, jnp.sum(do * o, axis=1, keepdims=True) * inv)
    do_ref[...] = (do * inv).astype(BF16)
    zero(acc_ref)

    def back_tile(j, _):
        r = keys(j)
        p = s_ref[:, r]
        dp = over_cols(do_ref[...], v_ref[r, :])
        ds = (p * (dp - wide(d_ref[...]))).astype(BF16)
        dv_ref[r, :] += over_rows(p.astype(BF16), do_ref[...])
        dk_ref[r, :] += over_rows(ds, q_ref[...])
        acc_ref[...] += exact(ds, k_ref[r, :])
        return 0

    lax.fori_loop(0, i + 1, back_tile, 0)
    dq = acc_ref[...] * scale
    turned = dq[:, nope:]
    turned = turned * cm_ref[...] - swapped(turned) * sm_ref[...]
    odq_ref[:, vd:vd + nope] = dq[:, :nope].astype(BF16)
    odq_ref[:, vd + nope:] = turned.astype(BF16)
    sent_ref[:, :half] = o.astype(BF16).reshape(-1, half, LANES)
    sent_ref[:, half:2 * half] = dq[:, :nope].astype(BF16).reshape(-1, half, LANES)
    turned = turned.reshape(-1, half, LANES)
    low, high = turned[:, :half // 2], turned[:, half // 2:]
    lane = lax.broadcasted_iota(jnp.int32, low.shape, 2)
    sent_ref[:, 2 * half:] = jnp.where(lane < rope, low, pltpu.roll(high, rope, 2)).astype(BF16)

    @pl.when(i == n - 1)
    def _():
        def finish(s, _):
            to = at_block(s, half)
            for ref, side in ((keep_ref, core), (give_ref, 1 - core)):
                r = at_block(2 * s + side, half)
                ref[to, :SLOT] = dk_ref[r, :] * scale
                ref[to, SLOT:] = dv_ref[r, :]
            return 0

        lax.fori_loop(0, dk_ref.shape[0] // shard, finish, 0)


def attention(place, x, far, near, w_dkv, wq, wr, gain, uk, uv, g, scale, shard, nope, rope, n):
    seq, d_model = x.shape
    rank, vd = w_dkv.shape[1], g.shape[1]
    half, nq, bk = shard // 2, seq // 2, seq // n
    bq = nq // n
    sent = seq // shard, 2 * half + half // 2, LANES
    vmem = lambda *shape: pltpu.VMEM(shape, F32)
    packed = lambda *shape: pltpu.VMEM(shape, BF16)
    return pl.pallas_call(
        functools.partial(attn_kernel, scale, shard, half, nope, rope),
        grid_spec=pltpu.PrefetchScalarGridSpec(
            num_scalar_prefetch=1, grid=(n,),
            in_specs=[rows(bk, d_model), whole(*far.shape), whole(*near.shape), whole(*w_dkv.shape), pl.BlockSpec((1, *wq.shape[1:]), lambda i, c: (c[1], 0, 0)),
                      whole(*wr.shape), whole(*gain.shape), whole(*uk.shape), whole(*uv.shape), rows(bq, vd)],
            out_specs=[rows(bq, vd + SLOT), pl.BlockSpec((sent[0] // n, *sent[1:]), lambda i, c: (i, 0, 0)), whole(nq, SLOT + vd), whole(nq, SLOT + vd), rows(bk, rank)],
            scratch_shapes=[packed(d_model, SLOT), packed(rank, nope + vd), packed(bq, SLOT), packed(seq, SLOT), packed(seq, vd),
                            vmem(bq, LANES), vmem(bq, LANES), vmem(bq, seq), vmem(bq, LANES), vmem(bq, LANES), packed(bq, vd), vmem(bq, LANES), vmem(bq, SLOT),
                            vmem(seq, SLOT), vmem(seq, vd)]),
        out_shape=[struct((nq, vd + SLOT), BF16), struct(sent, BF16), struct((nq, SLOT + vd)), struct((nq, SLOT + vd)), struct((seq, rank), BF16)],
        compiler_params=compiler_params(),
        cost_estimate=cost(2 * seq * d_model * (rank + SLOT) + 7 * nq * seq * SLOT, 2 * x.size, nq * seq),
    )(place, x, far, near, w_dkv, wq, wr, gain, uk, uv, g)


def ring_kernel(side, counts, make, n_given, n_made, *refs):
    n_ring, n_each, _ = counts
    total = sum(counts)
    given = refs[:n_given]
    srcs, outs = refs[n_given:n_given + total], refs[n_given + total:n_given + 2 * total + n_made]
    send_sem, recv_sem, own_sem, *rest = refs[n_given + 2 * total + n_made:]
    direct_sem, made = rest[:2], rest[2:]
    sent_to = [(srcs[k], outs[k], k < n_ring + n_each) for k in range(n_ring, total)]
    if make:
        sent_to.append((made[0], outs[total], True))
    n_dev = 2 * side * side
    me = lax.axis_index("cp")
    pos = ((me // 2) % side, me // (2 * side))
    mesh_id = pl.DeviceIdType.MESH

    def at(dx, dy):
        return (lax.rem(pos[1] + dy + side, side) * side + lax.rem(pos[0] + dx + side, side)) * 2 + me % 2

    def shifted(color, first, second):
        return at(second, first) if color else at(first, second)

    sibling = me + 1 - 2 * (me % 2)
    direct = len(sent_to) > 0
    neighbours = [shifted(color, d, 0) for color in range(2) for d in (1, -1)]
    barrier = pltpu.get_barrier_semaphore()

    def greet(peer):
        pl.semaphore_signal(barrier, inc=1, device_id={"cp": peer}, device_id_type=mesh_id)

    def others(do):
        def body(d, _):
            do(d)
            return 0

        lax.fori_loop(1, n_dev, body, 0)

    if direct:
        others(lambda d: greet(me ^ d))
        pl.semaphore_wait(barrier, n_dev - 1)
    else:
        for peer in (*neighbours, sibling):
            greet(peer)
        pl.semaphore_wait(barrier, len(neighbours) + 1)

    def part(ref, color, piece=0, pieces=1):
        size = ref.shape[0] // (2 * pieces)
        return ref.at[pl.ds((pieces * color + piece) * size, size)]

    def copy(src, dst, sems, peer):
        return pltpu.make_async_remote_copy(src_ref=src, dst_ref=dst, send_sem=sems[0], recv_sem=sems[1], device_id={"cp": peer}, device_id_type=mesh_id)

    def sems(k, color, event):
        return send_sem.at[k, color, event], recv_sem.at[k, color, event]

    pending = []

    def send(color, event, block, peer, *piece):
        for k in range(n_ring):
            src, dst = (srcs[k], outs[k].at[me]) if block is None else (outs[k].at[block],) * 2
            pending.append(copy(part(src, color, *piece), part(dst, color, *piece), sems(k, color, event), peer))
            pending[-1].start()

    def arrived(color, event, block, *piece):
        for k in range(n_ring):
            ref = part(outs[k].at[block], color, *piece)
            copy(ref, ref, sems(k, color, event), sibling).wait_recv()

    local = lambda src, dst, k: pltpu.make_async_copy(src, dst, own_sem.at[k])
    own = [local(srcs[k], outs[k].at[me], k) for k in range(n_ring)]
    late = [local(src.at[me] if each else src, dst.at[me], n_ring + k) for k, (src, dst, each) in enumerate(sent_to)]
    late += [local(made[k], outs[total + k], total + k) for k in range(1, n_made)]

    def straight(d):
        for k, (src, dst, each) in enumerate(sent_to):
            yield copy(src.at[me ^ d] if each else src, dst.at[me], [s.at[k, d] for s in direct_sem], me ^ d)

    def start_direct():
        for c in late:
            c.start()
        if direct:
            others(lambda d: [c.start() for c in straight(d)])

    def wait_all():
        for c in own + late:
            c.wait()
        if direct:
            others(lambda d: [c.wait() for c in straight(d)])

    for c in own:
        c.start()
    if not make:
        start_direct()
    finish = make(*given, *made) if make else None

    colors = range(2)
    offsets = (0, -1, 1, 2)
    first_out, relays, second_out, to_sibling, column = 0, 2, 4, 20, 24

    def spread(c, j, block):
        for d, way in enumerate((1, -1)):
            send(c, second_out + 4 * j + d, block, shifted(c, 0, way))
        send(c, to_sibling + j, block, sibling)

    def relay(c, j):
        for d, way in enumerate((1, -1)):
            block = shifted(c, offsets[j], -way)
            arrived(c, second_out + 4 * j + d, block)
            send(c, second_out + relays + 4 * j + d, block, shifted(c, 0, way), d, 2)
            send(c, column + 3 * j + d, block, sibling)

    if not n_ring:
        wait_all()
        return
    for c in colors:
        for d, way in enumerate((1, -1)):
            send(c, first_out + d, None, shifted(c, way, 0))
        spread(c, 0, None)
    for c in colors:
        for d, way in enumerate((1, -1)):
            block = shifted(c, -way, 0)
            arrived(c, first_out + d, block)
            send(c, relays + d, block, shifted(c, way, 0), d, 2)
            spread(c, 1 + d, block)
    for c in colors:
        relay(c, 0)
    if make:
        finish()
    for c in colors:
        across = shifted(c, 2, 0)
        for d in range(2):
            arrived(c, relays + d, across, d, 2)
        spread(c, 3, across)
    if make:
        start_direct()
    for j in range(1, 4):
        for c in colors:
            relay(c, j)
    for j in range(4):
        for c in colors:
            across = shifted(c, offsets[j], 2)
            for d in range(2):
                arrived(c, second_out + relays + 4 * j + d, across, d, 2)
            send(c, column + 2 + 3 * j, across, sibling)
    other = sibling - me
    for c in colors:
        for j in range(4):
            arrived(c, to_sibling + j, shifted(c, offsets[j], 0) + other)
            for d in range(3):
                arrived(c, column + 3 * j + d, shifted(c, offsets[j], offsets[1 + d]) + other)
    for c in pending:
        c.wait_send()
    wait_all()


def ring_gather(n_dev, cid, ring, each=(), same=(), make=None, given=(), made=(), scratch=()):
    side = round((n_dev // 2) ** 0.5)
    sent = [*ring, *each, *same]
    n_made = len(made)
    shapes = [struct(a.shape if len(ring) <= k < len(ring) + len(each) else (n_dev,) + a.shape, a.dtype) for k, a in enumerate(sent)]
    shapes += [struct(a.shape, a.dtype) for a in made]
    counts = len(ring), len(each), len(same)
    n_direct = sum(counts[1:]) + (1 if make else 0)
    dma = pltpu.SemaphoreType.DMA
    in_vmem, anywhere = pl.BlockSpec(memory_space=pltpu.VMEM), pl.BlockSpec(memory_space=pl.ANY)
    return pl.pallas_call(
        functools.partial(ring_kernel, side, counts, make, len(given), n_made),
        in_specs=[anywhere] * len(given) + [in_vmem] * len(sent), out_specs=[anywhere] * len(shapes), out_shape=shapes,
        scratch_shapes=[dma((max(len(ring), 1), 2, EVENTS))] * 2 + [dma((len(shapes),))] + [dma((max(n_direct, 1), n_dev))] * 2 + [*made, *scratch],
        compiler_params=compiler_params(collective_id=cid, has_side_effects=True),
        cost_estimate=cost(4e10),
    )(*given, *sent)


def make_early(gy_ref, w_ref, uk_ref, uv_ref, blocks_ref, uk_head_ref, uv_head_ref, *rest):
    *vmem, sems = rest
    reads = [pltpu.make_async_copy(src, dst, sems.at[k]) for k, (src, dst) in enumerate(zip((gy_ref, w_ref, uk_ref, uv_ref), vmem))]
    for c in reads:
        c.start()
    gy_vmem, w_vmem, uk_vmem, uv_vmem = vmem

    def compute():
        for c in reads:
            c.wait()
        heads, v_dim = w_ref.shape[:2]
        half = blocks_ref.shape[1]
        head = lax.axis_index("cp") // 2

        def two_heads(b, _):
            w = w_vmem[pl.ds(2 * b, 2)].reshape(2 * v_dim, -1)
            g = over_cols(gy_vmem[...], w).astype(BF16)
            for h in range(2):
                for core in range(2):
                    blocks_ref[4 * b + 2 * h + core] = g[core * half:(core + 1) * half, h * v_dim:(h + 1) * v_dim]
            return 0

        lax.fori_loop(0, heads // 2, two_heads, 0)

        def pick(b, _):
            r = at_block(b, LANES)
            for src, dst in ((uk_vmem, uk_head_ref), (uv_vmem, uv_head_ref)):
                w = src[r].astype(F32)
                dst[r, :] = jnp.sum(jnp.where(lax.broadcasted_iota(jnp.int32, w.shape, 1) == head, w, 0.0), axis=1).astype(BF16)
            return 0

        lax.fori_loop(0, uk_head_ref.shape[0] // LANES, pick, 0)

    return compute


def query_grads_kernel(qk_dim, core_ref, x_ref, odq_ref, keep_ref, give_ref, q_acc):
    i = pl.program_id(0)
    core = core_ref[0]
    d_model = x_ref.shape[-1]

    @pl.when(i == 0)
    def _():
        zero(q_acc)

    x = x_ref[...].reshape(-1, d_model)
    dq_t = odq_ref[...].T[-SLOT:][:qk_dim]
    for c in range(4):
        cols = slice(c * d_model // 4, (c + 1) * d_model // 4)
        q_acc[:, cols] += exact(dq_t, x[:, cols])

    @pl.when(i == pl.num_programs(0) - 1)
    def _():
        for ref, side in ((keep_ref, core), (give_ref, 1 - core)):
            ref[...] = q_acc[at_block(side, qk_dim // 2), :]


def output_grads_kernel(core_ref, gy_ref, odq_ref, keep_ref, give_ref, o_acc):
    i = pl.program_id(0)
    core = core_ref[0]
    vd, d_model = o_acc.shape

    @pl.when(i == 0)
    def _():
        zero(o_acc)

    gy = gy_ref[...].reshape(-1, d_model)
    o_t = odq_ref[...].T[:vd]
    for c in range(4):
        cols = slice(c * d_model // 4, (c + 1) * d_model // 4)
        o_acc[:, cols] += exact(o_t, gy[:, cols])

    @pl.when(i == pl.num_programs(0) - 1)
    def _():
        for ref, side in ((keep_ref, core), (give_ref, 1 - core)):
            ref[...] = o_acc[at_block(side, vd // 2), :]


def head_grads(kernel, core, act, odq, n_dev, half, width):
    n = 4
    shards = n_dev // n
    d_model = act.shape[1]
    out = width // 2, d_model
    return pl.pallas_call(
        kernel,
        grid_spec=pltpu.PrefetchScalarGridSpec(
            num_scalar_prefetch=1, grid=(n,),
            in_specs=[pl.BlockSpec((shards, 1, half, d_model), lambda i, c: (i, c[0], 0, 0)), rows(shards * half, odq.shape[1])],
            out_specs=[whole(*out)] * 2, scratch_shapes=[pltpu.VMEM((width, d_model), F32)]),
        out_shape=[struct(out)] * 2, compiler_params=compiler_params(), cost_estimate=cost(act.size * width, act.size),
    )(core[None], act.reshape(n_dev, 2, half, d_model), odq)


def up_grads_kernel(core_ref, latent_ref, kv_ref, keep_ref, give_ref):
    core = core_ref[0]
    up = over_rows(latent_ref[...].reshape(-1, latent_ref.shape[-1]), kv_ref[...])
    count = keep_ref.shape[0]
    width = up.shape[1]
    blocks = keep_ref.shape[1] // width
    for a in range(blocks):
        lo, hi = (up[(s * blocks + a) * count:(s * blocks + a + 1) * count] for s in range(2))
        cols = slice(a * width, (a + 1) * width)
        keep_ref[:, cols] = jnp.where(core == 0, lo, hi)
        give_ref[:, cols] = jnp.where(core == 0, hi, lo)


def up_grads(core, latent, kv, d_model, n_dev, half):
    rank, width = latent.shape[1], kv.shape[1]
    out = rank * width // (2 * d_model), d_model
    return pl.pallas_call(
        up_grads_kernel,
        grid_spec=pltpu.PrefetchScalarGridSpec(
            num_scalar_prefetch=1, grid=(1,),
            in_specs=[pl.BlockSpec((n_dev, 1, half, rank), lambda i, c: (0, c[0], 0, 0)), whole(*kv.shape)], out_specs=[whole(*out)] * 2),
        out_shape=[struct(out)] * 2, compiler_params=compiler_params(), cost_estimate=cost(2 * kv.size * rank, latent.size),
    )(core[None], latent.reshape(n_dev, 2, half, rank), kv)


def finish_kernel(x_ref, low_ref, g_ref, up_ref, dkv_ref, kr_ref, copy_ref, uk_ref, uv_ref, low_t):
    @pl.when(pl.program_id(0) == 0)
    def _():
        n_dev, _, shard = low_ref.shape
        for d in range(n_dev):
            low_t[:, d * shard:(d + 1) * shard] = low_ref[d]

    g = exact(low_t[...], x_ref[...])
    rank = dkv_ref.shape[1]
    dkv_ref[...] = g[:rank].T
    kr_ref[...] = g[rank:]
    copy_ref[...] = g_ref[...]
    spread_heads_kernel(up_ref, uk_ref, uv_ref)


def finish(x, low, g, up, rank, nope):
    seq, d_model = x.shape
    width = low.shape[1]
    rope = width - rank
    steps = 4
    cols = d_model // steps
    piece = rows(g.shape[0] // steps, g.shape[1])
    heads, _, count, width_up = up.shape
    head_rows = pl.BlockSpec((rank // steps, heads, nope), lambda i: (i, 0, 0))
    return pl.pallas_call(
        finish_kernel, grid=(steps,),
        in_specs=[pl.BlockSpec((seq, cols), lambda i: (0, i)), whole(*low.shape), piece,
                  pl.BlockSpec((heads, 1, count, width_up // 2), lambda i: (0, i // 2, 0, i % 2))],
        out_specs=[rows(cols, rank), pl.BlockSpec((rope, cols), lambda i: (0, i)), piece, head_rows, head_rows],
        out_shape=[struct((d_model, rank)), struct((rope, d_model)), struct(g.shape)] + [struct((rank, heads, nope))] * 2,
        scratch_shapes=[pltpu.VMEM((width, seq), BF16)],
        compiler_params=compiler_params(), cost_estimate=cost(2 * x.size * width, 2 * x.size + 8 * g.size),
    )(x, low, g, up)


def spread_heads_kernel(up_ref, uk_ref, uv_ref):
    heads, _, count, cols = up_ref.shape
    for a, block in enumerate(jnp.split(up_ref[...].reshape(heads, count, cols), cols // SLOT, axis=2)):
        for ref, value in zip((uk_ref, uv_ref), jnp.split(block, 2, axis=2)):
            ref[a * count:(a + 1) * count] = jnp.swapaxes(value, 0, 1)


def solution(mesh):
    n_dev = mesh.shape['cp']
    row_spec, per_group = P(('dp', 'cp')), P('dp')
    siblings = [(i, i ^ 1) for i in range(n_dev)]

    def block(x_loc, gy_loc, w_q, w_dkv, g_kv, w_kr, w_uk, w_uv, w_o):
        shard, d_model = x_loc.shape
        heads, qk_dim = w_q.shape[1:]
        rank, _, nope = w_uk.shape
        v_dim, rope = w_uv.shape[2], w_kr.shape[1]
        half, seq = shard // 2, n_dev * shard
        me = lax.axis_index('cp')
        head, core = me // 2, me % 2

        def gather(a):
            return lax.all_gather(a, 'cp', axis=0, tiled=True)

        def summed(keep, give):
            return keep + lax.ppermute(give, 'cp', siblings)

        packed = lambda *shape: pltpu.VMEM(shape, BF16)
        given = gy_loc, w_o, w_uk, w_uv
        x_all, d_out, uk, uv = ring_gather(n_dev, 1, [x_loc], make=make_early, given=given, made=(packed(n_dev, half, v_dim), packed(rank, nope), packed(rank, v_dim)),
                                           scratch=[*(packed(*a.shape) for a in given), pltpu.SemaphoreType.DMA((len(given),))])
        x_all, d_out = x_all.reshape(seq, d_model), d_out.reshape(seq // 2, v_dim)
        gy_all = gather(lax.optimization_barrier((gy_loc, x_all))[0])


        def table(positions):
            return np.concatenate([t for t in rope_tables(positions.astype(np.float32), rope, np) for _ in range(LANES // rope)], axis=1)

        far, near = table(np.arange(0, seq, 4 * shard)), table(np.arange(4 * shard))
        gain = g_kv.astype(F32)[None]
        odq, sent, kv_keep, kv_give, latent = attention(jnp.stack([core, head]), x_all, far, near, w_dkv, w_q.transpose(1, 2, 0), w_kr.T, gain, uk, uv, d_out, qk_dim ** -0.5, shard, nope, rope, 4)

        def exchange(a):
            return lax.all_to_all(a, 'cp', 0, 0, tiled=True).reshape(heads, 2, *a.shape[1:])

        q_keep, q_give = head_grads(functools.partial(query_grads_kernel, qk_dim), core, x_all, odq, n_dev, half, qk_dim)
        got_odq = exchange(lax.optimization_barrier((sent, q_keep))[0])
        q_my = summed(q_keep, q_give)
        gwq = gather(q_my)

        kv_sum = lax.optimization_barrier((summed(kv_keep, kv_give), q_keep))[0]
        kv_my = jnp.concatenate([kv_sum[:, :nope], kv_sum[:, SLOT:]], axis=1).astype(BF16)
        dkr_my = kv_sum[:, nope:qk_dim].reshape(n_dev, half * rope // LANES, LANES)
        o_keep, o_give = head_grads(output_grads_kernel, core, gy_all, odq, n_dev, half, v_dim)
        o_my = summed(o_keep, o_give)
        gwo = gather(o_my)
        got_odq, kv_my, _ = lax.optimization_barrier((got_odq, kv_my, o_keep))
        got_kv = exchange(kv_my.reshape(n_dev, half, -1))
        dkr_my = lax.optimization_barrier((dkr_my, o_my))[0]
        got_r, = ring_gather(n_dev, 2, [], [dkr_my])
        got_odq, got_r, kv_my = lax.optimization_barrier((got_odq, got_r, kv_my))
        up_keep, up_give = up_grads(core, latent, kv_my, d_model, n_dev, half)
        up_my = summed(up_keep, up_give)
        o_loc, dq_loc, dq_rope = jnp.split(got_odq, [half, 2 * half], axis=2)
        dq_loc = jnp.concatenate([dq_loc, jnp.concatenate([dq_rope[..., :rope], dq_rope[..., rope:]], axis=2)], axis=3)
        o_loc, dq_loc = o_loc.reshape(heads, shard, -1), dq_loc.reshape(heads, shard, -1)
        y_loc = jnp.einsum('htv,hvd->td', o_loc, w_o, preferred_element_type=F32).astype(BF16)
        dx_loc = jnp.einsum('hte,dhe->td', dq_loc, w_q, preferred_element_type=F32)
        got_kv, got_r, y_loc, dx_loc = lax.optimization_barrier((got_kv, got_r, y_loc, dx_loc))
        dkr_loc = jnp.sum(got_r.reshape(heads, shard, rope), axis=0)
        dk_loc, dv_loc = jnp.split(got_kv.reshape(heads, shard, -1), [nope], axis=2)
        d_latent = jnp.einsum('htn,chn->tc', dk_loc, w_uk, preferred_element_type=F32) + jnp.einsum('htv,chv->tc', dv_loc, w_uv, preferred_element_type=F32)
        c_loc = exact(x_loc, w_dkv)
        inv_loc = lax.rsqrt(jnp.mean(c_loc * c_loc, axis=-1, keepdims=True) + NORM_EPS)
        c_norm = c_loc * inv_loc
        gg_part = jnp.sum(d_latent * c_norm, axis=0)
        d_norm = d_latent * gain
        dc_loc = (inv_loc * (d_norm - c_norm * jnp.mean(d_norm * c_norm, axis=-1, keepdims=True))).astype(BF16)
        cos_t, sin_t = rope_tables((me * shard + jnp.arange(shard)).astype(F32), rope)
        dkr_raw = rope_back(dkr_loc, cos_t, sin_t).astype(BF16)
        dx_loc = dx_loc + jnp.einsum('tc,dc->td', dc_loc, w_dkv, preferred_element_type=F32) + jnp.einsum('tr,dr->td', dkr_raw, w_kr, preferred_element_type=F32)

        gg_rows = rank // LANES
        gg_part = jnp.pad(gg_part.reshape(gg_rows, LANES), ((0, 8 - gg_rows), (0, 0)))
        low_my = jnp.concatenate([dc_loc, dkr_raw], axis=1).T
        low_my, dx_loc = lax.optimization_barrier((low_my, dx_loc.astype(BF16)))
        low, up, gg = ring_gather(n_dev, 3, [low_my, up_my], (), [gg_part])
        gw_dkv, gw_kr, gwq, gw_uk, gw_uv = finish(x_all, low, gwq, up.reshape(heads, 2, -1, d_model), rank, nope)
        gg_kv = jnp.sum(gg, axis=0)[:gg_rows].reshape(rank)
        gw_q = gwq.reshape(heads, qk_dim, d_model).transpose(2, 0, 1)
        return y_loc, dx_loc, gw_q, gw_dkv, gg_kv, gw_kr.T, gw_uk, gw_uv, gwo.reshape(heads, v_dim, d_model)

    return jax.shard_map(block, mesh=mesh, in_specs=(row_spec, row_spec) + (P(),) * 7, out_specs=(row_spec, row_spec) + (per_group,) * 7, check_vma=False)
```
